256 devices in a mesh: dp: 16 (over z, core), feat: 16 (over x, y).
Axes of the slice: x: 4, y: 4, z: 8, core: 2. Of those that a mesh axis runs over, the one named last changes fastest.
Arguments:
- points: bfloat16 [4096, 256], P('dp'), may hold values from -6 to 6
- freqs: bfloat16 [256, 8192], P(None, 'feat'), may hold values from -0.375 to 0.375
- phase: float32 [8192], P('feat'), may hold values from -3.140625 to 3.140625
- ridge: float32 [8192], P('feat'), may hold values from 0.05 to 0.5
- targets: bfloat16 [8, 4096], P(None, 'dp'), may hold values from -6 to 6
Outputs:
- gram: float32 [8192, 8192], P('feat', 'dp')
- projected: float32 [8, 8192], P(None, 'feat')
- factors: float32 [8192, 1024], P('feat')
The draws below stay inside these ranges and needn't reach their ends.
All inputs are finite; a program needn't handle non-finite values.
Results may differ from the reference program's by a relative error of at most 0.003.
Values may be sent and summed in bfloat16 or wider, within the bound.
No kernel may reach another device: no remote copies, remote signals or barrier semaphores. Data moves between devices by JAX's collectives and lax.ppermute only.
A program may use at most 128 MiB of HBM per device.

```python
import math
import jax
import jax.numpy as jnp
from jax import lax

DIN = 256
OUTS = 8
FB = 1024
F = 8192
ROWS = 4096


def steps_of(rng, shape, pieces, smallest, top_value):
    def one(position, blocks):
        steps = jax.random.uniform(jax.random.fold_in(jax.random.fold_in(rng, 6), position), (blocks,), jnp.float32, smallest / len(pieces), top_value / len(pieces))
        return jnp.repeat(jnp.exp(steps), shape[position] // blocks).reshape((-1,) + (1,) * (len(shape) - position - 1))

    gain = one(*pieces[0])
    for cut in pieces[1:]:
        gain = gain * one(*cut)
    return gain


def gaussian(own_key, extent, spread, limit, cuts=(), held_as=jnp.bfloat16):
    array = jax.random.normal(own_key, extent, jnp.float32) * spread
    if len(cuts) > 0:
        array = steps_of(own_key, extent, cuts, -0.22, 0.18) * array
    return jnp.clip(array, min=-limit, max=limit).astype(held_as)


def setup_inputs(seed: int = 0) -> dict:
    keys = jax.random.split(jax.random.key(seed), 6)
    points = gaussian(keys[0], (ROWS, DIN), 1.0, 6.0, ((0, 16),))
    freqs = gaussian(keys[1], (DIN, F), DIN ** -0.5, 0.375, ((1, 16),))
    phase = jnp.clip(jax.random.uniform(keys[2], (F,), jnp.float32, -3.140625, 3.140625), -3.140625, 3.140625)
    ridge = jnp.clip(jnp.exp(math.log(0.5) - 2.3025851 * jax.random.uniform(keys[3], (F,), jnp.float32) ** steps_of(keys[3], (F,), ((0, 16),), -0.2, 0.2)), 0.05, 0.5)
    targets = gaussian(keys[4], (OUTS, ROWS), 1.0, 6.0, ((1, 16),))
    return {"points": points, "freqs": freqs, "phase": phase, "ridge": ridge, "targets": targets}


def reference(points, freqs, phase, ridge, targets):
    scale = math.sqrt(2.0 / ROWS)
    angle = jnp.dot(points.astype(jnp.float32), freqs.astype(jnp.float32), preferred_element_type=jnp.float32) + phase
    phi = (scale * jnp.cos(angle)).astype(jnp.bfloat16)
    phi_wide = phi.astype(jnp.float32)
    gram = jnp.dot(phi_wide.T, phi_wide, precision=lax.Precision.HIGHEST) + jnp.diag(ridge)
    projected = jnp.dot(targets.astype(jnp.float32), phi_wide, precision=lax.Precision.HIGHEST)
    blocks = jnp.stack([gram[block_number * FB:(block_number + 1) * FB, block_number * FB:(block_number + 1) * FB] for block_number in range(OUTS)])
    factors = jnp.linalg.cholesky(blocks).reshape(F, FB)
    return (gram, projected, factors)
```

```python
import functools
import math

import jax
import jax.numpy as jnp
from jax import lax
from jax.experimental import pallas as pl
from jax.experimental.pallas import tpu as pltpu
from jax.sharding import PartitionSpec as P

FB = 1024
B = 128
b = 16

def lane(x, c):
    return jnp.broadcast_to(x[:, c:c + 1], (x.shape[0], B))

def chain(rt, ut):
    rows = lax.broadcasted_iota(jnp.int32, (b, B), 0)
    for o in range(0, B, b):
        rd = rt[o:o + b, :B]
        ri = rt[o:o + b, B:]
        C = [lane(rd, o + k) for k in range(b)]
        nxt = min(b, B - o - b)
        if nxt:
            nd = rt[o + b:o + b + nxt, :B]
            F = [lane(nd, o + k) for k in range(b)]
        rv = jnp.zeros((b, B), jnp.float32)
        for k in range(b):
            ck = C[k]
            rs = lax.rsqrt(ck[k:k + 1, :])
            m = rows == k
            lz = jnp.where(m, 0.0, ck) * rs
            ud = rd[k:k + 1, :] * rs
            ui = ri[k:k + 1, :] * rs
            ut[o + k:o + k + 1, :B] = ud
            ut[o + k:o + k + 1, B:] = ui
            for j in range(k + 1, b):
                C[j] = C[j] - lz * (C[j][k:k + 1, :] * rs)
            rd = rd - lz * ud
            ri = ri - lz * ui
            rv = jnp.where(m, rs * rs, rv)
        if nxt:
            rd = rd * rv
            ri = ri * rv
            VD = [rd[k:k + 1, :] for k in range(b)]
            VI = [ri[k:k + 1, :] for k in range(b)]
            for g in range(o + b, B, b):
                xd = rt[g:g + b, :B]
                xi = rt[g:g + b, B:]
                G = F if g == o + b else [lane(xd, o + k) for k in range(b)]
                for k in range(b):
                    xd = xd - G[k] * VD[k]
                    xi = xi - G[k] * VI[k]
                rt[g:g + b, :B] = xd
                rt[g:g + b, B:] = xi

def split3(x):
    x1 = x.astype(jnp.bfloat16)
    r = x - x1.astype(jnp.float32)
    x2 = r.astype(jnp.bfloat16)
    x3 = (r - x2.astype(jnp.float32)).astype(jnp.bfloat16)
    return x1, x2, x3

def nt(x, y):
    return lax.dot_general(x, y, (((1,), (1,)), ((), ())), preferred_element_type=jnp.float32)

def nt6(x, y):
    l = jnp.concatenate([x[0], x[0], x[1], x[1], x[0], x[2]], axis=1)
    r = jnp.concatenate([y[0], y[1], y[0], y[1], y[2], y[0]], axis=1)
    return nt(l, r)

def chol_kernel(h_ref, a_ref, o_ref, rt, ut, L, S1, S2, S3, *, n):
    nb = n // B
    tri = lax.broadcasted_iota(jnp.int32, (B, B), 0) >= lax.broadcasted_iota(jnp.int32, (B, B), 1)
    eye = (lax.broadcasted_iota(jnp.int32, (B, B), 0) == lax.broadcasted_iota(jnp.int32, (B, B), 1)).astype(jnp.float32)
    rt[:, :B] = a_ref[0:B, 0:B]
    for j in range(nb):
        L[j * B:(j + 1) * B, :] = jnp.zeros((B, n), jnp.float32)

    def step(kk, carry):
        rt[:, B:] = eye
        chain(rt, ut)
        for j in range(nb):
            @pl.when(kk == j)
            def _():
                lo = j * B
                ljj = jnp.where(tri, ut[:, :B].T, 0.0)
                L[lo:lo + B, lo:lo + B] = ljj
                if j + 1 < nb:
                    hi = lo + B
                    minv = jnp.where(tri, ut[:, B:], 0.0)
                    ms = split3(minv)
                    w = a_ref[hi:n, lo:hi]
                    if j:
                        w = w - nt6([s[hi:n, 0:lo] for s in (S1, S2, S3)],
                                    [s[lo:hi, 0:lo] for s in (S1, S2, S3)])
                    x = nt6(split3(w), ms)
                    L[hi:n, lo:hi] = x
                    xs = split3(x)
                    S1[hi:n, lo:hi], S2[hi:n, lo:hi], S3[hi:n, lo:hi] = xs
                    d = nt6([s[hi:hi + B, 0:hi] for s in (S1, S2, S3)],
                            [s[hi:hi + B, 0:hi] for s in (S1, S2, S3)])
                    rt[:, :B] = a_ref[hi:hi + B, hi:hi + B] - d
        return carry
    lax.fori_loop(0, nb, step, 0)
    o_ref[...] = L[pl.ds(pl.multiple_of(h_ref[0] * (n // 2), n // 2), n // 2), :]

def chol(a, h):
    n = a.shape[0]
    return pl.pallas_call(
        functools.partial(chol_kernel, n=n),
        out_shape=jax.ShapeDtypeStruct((n // 2, n), jnp.float32),
        in_specs=[pl.BlockSpec(memory_space=pltpu.SMEM), pl.BlockSpec(memory_space=pltpu.VMEM)],
        out_specs=pl.BlockSpec(memory_space=pltpu.VMEM),
        scratch_shapes=[pltpu.VMEM((B, 2 * B), jnp.float32), pltpu.VMEM((B, 2 * B), jnp.float32),
                        pltpu.VMEM((n, n), jnp.float32)] + [pltpu.VMEM((n, n), jnp.bfloat16)] * 3,
        compiler_params=pltpu.CompilerParams(vmem_limit_bytes=48 * 2**20),
    )(h, a)

SIN = (6.28318516, -41.34165503, 81.60100407, -76.54978229, 39.53670602)


def features(rows, freq_cols, phase_turns, scale):
    dot = jnp.dot(rows, freq_cols, preferred_element_type=jnp.float32)
    turns = dot * (0.5 / math.pi) + phase_turns
    v = 0.25 - jnp.abs(turns - jnp.round(turns))
    w = v * v
    poly = scale * SIN[4]
    for c in SIN[3::-1]:
        poly = poly * w + scale * c
    return (v * poly).astype(jnp.bfloat16)


def cross(left, right):
    return lax.dot_general(
        left, right, (((0,), (0,)), ((), ())), preferred_element_type=jnp.float32
    )


def with_ridge(tile, ridge, row_start, col_start):
    rows_here = row_start + lax.broadcasted_iota(jnp.int32, tile.shape, 0)
    cols_here = col_start + lax.broadcasted_iota(jnp.int32, tile.shape, 1)
    return tile + jnp.where(rows_here == cols_here, ridge[:, None], 0.0)


def shards(points, freqs, phase, ridge, targets):
    nd = lax.axis_size("dp")
    nf = lax.axis_size("feat")
    fi = lax.axis_index("feat")
    di = lax.axis_index("dp")
    nz = nd // 2
    scale = math.sqrt(2.0 / (points.shape[0] * nd))
    rows = points.shape[0]

    def zshift(x, s):
        return lax.ppermute(x, "dp", [(2 * z + c, 2 * ((z + s) % nz) + c) for z in range(nz) for c in range(2)])

    def sibling(x):
        return lax.ppermute(x, "dp", [(i, i ^ 1) for i in range(nd)])

    def partner(x):
        return lax.ppermute(x, "feat", [(i, i ^ 1) for i in range(nf)])

    def swap(x):
        return lax.ppermute(x, ("dp", "feat"), [(i * nf + j, j * nd + i) for i in range(nd) for j in range(nf)])

    turns = phase * (0.5 / math.pi)
    small = jnp.stack([turns, ridge])
    pack = jnp.concatenate([points, targets], axis=0)
    freqs_p = partner(freqs)
    small_p = partner(small)
    chunks = [pack]
    up = down = pack
    for _ in range(nz // 2 - 1):
        up, down = zshift(up, 1), zshift(down, -1)
        chunks += [up, down]
    chunks.append(zshift(up, 1))
    chunks += [sibling(x) for x in chunks]
    points_all = jnp.concatenate([x[:rows] for x in chunks], axis=0)
    targets_all = jnp.concatenate([x[rows:] for x in chunks], axis=1)
    freqs_c = swap(freqs)
    small_c = swap(small)

    odd = fi % 2
    lo = odd == 0
    wf = jnp.concatenate([jnp.where(lo, freqs, freqs_p), jnp.where(lo, freqs_p, freqs)], axis=1)
    ws = jnp.concatenate([jnp.where(lo, small, small_p), jnp.where(lo, small_p, small)], axis=1)
    window_phi = features(points_all, wf, ws[0], scale)
    slab = with_ridge(cross(window_phi, window_phi), ws[1], 0, 0)
    factor_rows = chol(slab, jnp.reshape(odd, (1,)).astype(jnp.int32))
    row_phi = lax.dynamic_slice_in_dim(window_phi, odd * freqs.shape[1], freqs.shape[1], 1)
    projected = jnp.dot(targets_all, row_phi, preferred_element_type=jnp.float32)
    col_phi = features(points_all, freqs_c, small_c[0], scale)
    gram_tile = with_ridge(cross(row_phi, col_phi), ridge, fi * freqs.shape[1], di * freqs_c.shape[1])
    return (gram_tile, projected, factor_rows)


def solution(mesh):
    in_specs = (P("dp", None), P(None, "feat"), P("feat"), P("feat"), P(None, "dp"))
    out_specs = (P("feat", "dp"), P(None, "feat"), P("feat", None))
    return jax.shard_map(shards, mesh=mesh, in_specs=in_specs, out_specs=out_specs, check_vma=False)
```

```python
import functools
import math

import jax
import jax.numpy as jnp
from jax import lax
from jax.experimental import pallas as pl
from jax.experimental.pallas import tpu as pltpu
from jax.sharding import PartitionSpec as P

B = 128
NT = 256
VM = pl.BlockSpec(memory_space=pltpu.VMEM)
SM = pl.BlockSpec(memory_space=pltpu.SMEM)
SIN = (6.28318516, -41.34165503, 81.60100407, -76.54978229, 39.53670602)
b = 16

def lane(x, c):
    return jnp.broadcast_to(x[:, c:c + 1], (x.shape[0], B))

def chain(rt, ut):
    rows = lax.broadcasted_iota(jnp.int32, (b, B), 0)
    for o in range(0, B, b):
        rd = rt[o:o + b, :B]
        ri = rt[o:o + b, B:]
        C = [lane(rd, o + k) for k in range(b)]
        nxt = min(b, B - o - b)
        if nxt:
            nd = rt[o + b:o + b + nxt, :B]
            F = [lane(nd, o + k) for k in range(b)]
        rv = jnp.zeros((b, B), jnp.float32)
        for k in range(b):
            ck = C[k]
            rs = lax.rsqrt(ck[k:k + 1, :])
            m = rows == k
            lz = jnp.where(m, 0.0, ck) * rs
            ud = rd[k:k + 1, :] * rs
            ui = ri[k:k + 1, :] * rs
            ut[o + k:o + k + 1, :B] = ud
            ut[o + k:o + k + 1, B:] = ui
            for j in range(k + 1, b):
                C[j] = C[j] - lz * (C[j][k:k + 1, :] * rs)
            rd = rd - lz * ud
            ri = ri - lz * ui
            rv = jnp.where(m, rs * rs, rv)
        if nxt:
            rd = rd * rv
            ri = ri * rv
            VD = [rd[k:k + 1, :] for k in range(b)]
            VI = [ri[k:k + 1, :] for k in range(b)]
            for g in range(o + b, B, b):
                xd = rt[g:g + b, :B]
                xi = rt[g:g + b, B:]
                G = F if g == o + b else [lane(xd, o + k) for k in range(b)]
                for k in range(b):
                    xd = xd - G[k] * VD[k]
                    xi = xi - G[k] * VI[k]
                rt[g:g + b, :B] = xd
                rt[g:g + b, B:] = xi

def split3(x):
    x1 = x.astype(jnp.bfloat16)
    r = x - x1.astype(jnp.float32)
    x2 = r.astype(jnp.bfloat16)
    x3 = (r - x2.astype(jnp.float32)).astype(jnp.bfloat16)
    return x1, x2, x3

def nt(x, y):
    return lax.dot_general(x, y, (((1,), (1,)), ((), ())), preferred_element_type=jnp.float32)

def nt6(x, y):
    l = jnp.concatenate([x[0], x[0], x[1], x[1], x[0], x[2]], axis=1)
    r = jnp.concatenate([y[0], y[1], y[0], y[1], y[2], y[0]], axis=1)
    return nt(l, r)


def chol_kernel(h_ref, g0, g1, e0, e1, sm, sp, o_ref, rt, ut, L, S1, S2, S3, *, n):
    nb = n // B
    half = n // 2
    first = h_ref[0] == 0
    ii = lax.broadcasted_iota(jnp.int32, (B, B), 0)
    jj = lax.broadcasted_iota(jnp.int32, (B, B), 1)
    tri = ii >= jj
    eye = (ii == jj).astype(jnp.float32)

    def a(r0, r1, lo):
        if lo < half:
            return g0[r0:r1, lo:lo + B] + e0[r0:r1, lo:lo + B]
        return g1[r0 - half:r1 - half, lo - half:lo - half + B] + e1[r0 - half:r1 - half, lo - half:lo - half + B]

    def diag(lo):
        at = lo % half
        mine, other = sm[1:2, at:at + B], sp[1:2, at:at + B]
        row = jnp.where(first, mine, other) if lo < half else jnp.where(first, other, mine)
        return a(lo, lo + B, lo) + jnp.where(ii == jj, row, 0.0)

    rt[:, :B] = diag(0)
    for j in range(nb):
        L[j * B:(j + 1) * B, :] = jnp.zeros((B, n), jnp.float32)

    def step(kk, carry):
        rt[:, B:] = eye
        chain(rt, ut)
        for j in range(nb):
            @pl.when(kk == j)
            def _():
                lo = j * B
                ljj = jnp.where(tri, ut[:, :B].T, 0.0)
                L[lo:lo + B, lo:lo + B] = ljj
                if j + 1 < nb:
                    hi = lo + B
                    ms = split3(jnp.where(tri, ut[:, B:], 0.0))
                    w = a(hi, n, lo)
                    if j:
                        w = w - nt6([s[hi:n, 0:lo] for s in (S1, S2, S3)],
                                    [s[lo:hi, 0:lo] for s in (S1, S2, S3)])
                    x = nt6(split3(w), ms)
                    L[hi:n, lo:hi] = x
                    S1[hi:n, lo:hi], S2[hi:n, lo:hi], S3[hi:n, lo:hi] = split3(x)
                    d = nt6([s[hi:hi + B, 0:hi] for s in (S1, S2, S3)],
                            [s[hi:hi + B, 0:hi] for s in (S1, S2, S3)])
                    rt[:, :B] = diag(hi) - d
        return carry
    lax.fori_loop(0, nb, step, 0)
    o_ref[...] = L[pl.ds(pl.multiple_of(h_ref[0] * half, half), half), :]


def chol(h, parts, sm, sp):
    n = parts[0].shape[0]
    return pl.pallas_call(
        functools.partial(chol_kernel, n=n),
        out_shape=jax.ShapeDtypeStruct((n // 2, n), jnp.float32),
        in_specs=[SM] + [VM] * 6,
        out_specs=VM,
        scratch_shapes=[pltpu.VMEM((B, 2 * B), jnp.float32), pltpu.VMEM((B, 2 * B), jnp.float32),
                        pltpu.VMEM((n, n), jnp.float32)] + [pltpu.VMEM((n, n), jnp.bfloat16)] * 3,
        cost_estimate=pl.CostEstimate(flops=20 * 10**9, bytes_accessed=8 * 2**20, transcendentals=0),
        compiler_params=pltpu.CompilerParams(vmem_limit_bytes=40 * 2**20),
    )(h, *parts, sm, sp)


def feat(pts, wf, turns, scale):
    dot = jnp.dot(pts, wf, preferred_element_type=jnp.float32)
    t = dot * (0.5 / math.pi) + turns
    v = 0.25 - jnp.abs(t - jnp.round(t))
    w = v * v
    poly = w * (scale * SIN[4]) + scale * SIN[3]
    for c in SIN[2::-1]:
        poly = poly * w + scale * c
    return (v * poly).astype(jnp.bfloat16)


def tn(x, y):
    return lax.dot_general(x, y, (((0,), (0,)), ((), ())), preferred_element_type=jnp.float32)


def win_kernel(*refs, nc, acc, scale, half, rows):
    h_ref, fr, fp, sm, sp = refs[:5]
    chunks = refs[5:5 + nc]
    k = 5 + nc
    if acc:
        a0, a1 = refs[k:k + 2]
        k += 2
    g0, g1, pf, phi = refs[k:]
    first = h_ref[0] == 0
    for i in range(nc):
        pts = chunks[i][:rows, :]
        for c in range(0, half, NT):
            s = slice(c, c + NT)
            lo = jnp.where(first, fr[:, s], fp[:, s])
            hi = jnp.where(first, fp[:, s], fr[:, s])
            tlo = jnp.where(first, sm[0:1, s], sp[0:1, s])
            thi = jnp.where(first, sp[0:1, s], sm[0:1, s])
            phi[i * rows:(i + 1) * rows, c:c + NT] = feat(pts, lo, tlo, scale)
            phi[i * rows:(i + 1) * rows, half + c:half + c + NT] = feat(pts, hi, thi, scale)
    pf[...] = phi[:, pl.ds(pl.multiple_of(h_ref[0] * half, half), half)]
    for c in range(0, 2 * half, NT):
        lo = 0 if c < half else half
        out, at = (g0, c) if c < half else (g1, c - half)
        r = tn(phi[:, lo:], phi[:, c:c + NT])
        if acc:
            r = r + (a0 if c < half else a1)[:, at:at + NT]
        out[:, at:at + NT] = r


def win(h, fr, fp, sm, sp, chunks, acc, scale, rows):
    din, half = fr.shape
    nc = len(chunks)
    args = [h, fr, fp, sm, sp] + list(chunks) + list(acc or [])
    f32 = jnp.float32
    return pl.pallas_call(
        functools.partial(win_kernel, nc=nc, acc=acc is not None, scale=scale, half=half, rows=rows),
        out_shape=[jax.ShapeDtypeStruct((2 * half, half), f32), jax.ShapeDtypeStruct((half, half), f32),
                   jax.ShapeDtypeStruct((nc * rows, half), jnp.bfloat16)],
        in_specs=[SM] + [VM] * (len(args) - 1),
        out_specs=[VM] * 3,
        scratch_shapes=[pltpu.VMEM((nc * rows, 2 * half), jnp.bfloat16)],
        cost_estimate=pl.CostEstimate(flops=nc * rows * 2 * half * (din + 3 * half // 2) * 2,
                                      bytes_accessed=4 * 2**20, transcendentals=0),
        compiler_params=pltpu.CompilerParams(vmem_limit_bytes=32 * 2**20),
    )(*args)


def col_kernel(f_ref, fc, sc, sm, o1, o2, s1, s2, sib, *refs, scale, rows, stride):
    own = refs[:-3]
    g, pr, phi = refs[-3:]
    nc = len(own)
    width = fc.shape[1]
    parts = [o1, o2, s1, s2]
    tg = []
    for i in range(2 * nc):
        src = own[i] if i < nc else sib
        at = 0 if i < nc else (i - nc) * stride
        for c in range(0, width, NT):
            phi[i * rows:(i + 1) * rows, c:c + NT] = feat(src[at:at + rows, :], fc[:, c:c + NT], sc[0:1, c:c + NT], scale)
        tg.append(src[at + rows:at + rows + 16, :][:8])
    ii = lax.broadcasted_iota(jnp.int32, (width, NT), 0)
    jj = lax.broadcasted_iota(jnp.int32, (width, NT), 1)
    same = f_ref[0] != 0
    for c in range(0, width, NT):
        total = jnp.where((ii == jj + c) & same, sm[1:2, c:c + NT], 0.0)
        at = 0
        for p in parts:
            m = p.shape[0]
            total = total + tn(p[...], phi[at:at + m, c:c + NT])
            at += m
        g[:, c:c + NT] = total
    total = jnp.zeros((8, width), jnp.float32)
    at = 0
    for p in parts:
        m = p.shape[0] // rows
        total = total + jnp.dot(jnp.concatenate(tg[at:at + m], axis=1), p[...], preferred_element_type=jnp.float32)
        at += m
    pr[...] = total


def col(flag, fc, sc, sm, parts, sib, own, scale, rows):
    width = fc.shape[1]
    args = [flag, fc, sc, sm, *parts, sib, *own]
    total = sum(p.shape[0] for p in parts)
    return pl.pallas_call(
        functools.partial(col_kernel, scale=scale, rows=rows, stride=own[0].shape[0]),
        out_shape=[jax.ShapeDtypeStruct((parts[0].shape[1], width), jnp.float32),
                   jax.ShapeDtypeStruct((8, parts[0].shape[1]), jnp.float32)],
        in_specs=[SM] + [VM] * (len(args) - 1),
        out_specs=[VM] * 2,
        scratch_shapes=[pltpu.VMEM((total, width), jnp.bfloat16)],
        cost_estimate=pl.CostEstimate(flops=8 * 10**9, bytes_accessed=12 * 2**20, transcendentals=0),
        compiler_params=pltpu.CompilerParams(vmem_limit_bytes=40 * 2**20),
    )(*args)


def prep_kernel(p, t, ph, ri, pack, sm):
    rows = p.shape[0]
    pack[:rows, :] = p[...]
    pack[rows:, :] = jnp.concatenate([t[...], jnp.zeros_like(t[...])], axis=0)
    sm[...] = jnp.concatenate([ph[...] * (0.5 / math.pi), ri[...], jnp.zeros((6, ph.shape[1]), jnp.float32)], axis=0)


def prep(points, targets, phase, ridge):
    rows, din = points.shape
    w = phase.shape[0]
    return pl.pallas_call(
        prep_kernel,
        out_shape=[jax.ShapeDtypeStruct((rows + 16, din), jnp.bfloat16), jax.ShapeDtypeStruct((8, w), jnp.float32)],
        in_specs=[VM] * 4,
        out_specs=[VM] * 2,
    )(points, targets, phase.reshape(1, w), ridge.reshape(1, w))


def shards(points, freqs, phase, ridge, targets):
    nd = lax.axis_size("dp")
    nf = lax.axis_size("feat")
    fi = lax.axis_index("feat")
    di = lax.axis_index("dp")
    nz = nd // 2
    rows = points.shape[0]
    scale = math.sqrt(2.0 / (rows * nd))

    def zshift(x, s):
        return lax.ppermute(x, "dp", [(2 * z + c, 2 * ((z + s) % nz) + c) for z in range(nz) for c in range(2)])

    def sibling(x):
        return lax.ppermute(x, "dp", [(i, i ^ 1) for i in range(nd)])

    def partner(x):
        return lax.ppermute(x, "feat", [(i, i ^ 1) for i in range(nf)])

    def swap(x):
        return lax.ppermute(x, ("dp", "feat"), [(i * nf + j, j * nd + i) for i in range(nd) for j in range(nf)])

    pack, small = prep(points, targets, phase, ridge)
    fp = partner(freqs)
    u1, d1, u2, d2 = zshift(pack, 1), zshift(pack, -1), zshift(pack, 2), zshift(pack, -2)
    sp = partner(small)
    u3, d3, u4 = zshift(u2, 1), zshift(d2, -1), zshift(u2, 2)
    h = jnp.reshape(fi % 2, (1,)).astype(jnp.int32)
    first = [pack, u1, d1, u2, d2]
    last = [u3, d3, u4]
    g0, g1, pf1 = win(h, freqs, fp, small, sp, first, None, scale, rows)
    g0, g1, pf2 = win(h, freqs, fp, small, sp, last, (g0, g1), scale, rows)
    e0, e1 = sibling(g0), sibling(g1)
    late, lsm, o1, o2, own = lax.optimization_barrier((freqs, small, pf1, pf2, first + last + [e0]))
    own = own[:-1]
    fc, sc = swap(late), swap(lsm)
    sib = sibling(jnp.concatenate(own, axis=0))
    s1, s2 = sibling(o1), sibling(o2)
    factor_rows = chol(h, (g0, g1, e0, e1), small, sp)
    flag = jnp.reshape(fi == di, (1,)).astype(jnp.int32)
    gram_tile, projected = col(flag, fc, sc, small, (o1, o2, s1, s2), sib, own, scale, rows)
    return (gram_tile, projected, factor_rows)


def solution(mesh):
    in_specs = (P("dp", None), P(None, "feat"), P("feat"), P("feat"), P(None, "dp"))
    out_specs = (P("feat", "dp"), P(None, "feat"), P("feat", None))
    return jax.shard_map(shards, mesh=mesh, in_specs=in_specs, out_specs=out_specs, check_vma=False)
```

```python
import functools
import math

import jax
import jax.numpy as jnp
from jax import lax
from jax.experimental import pallas as pl
from jax.experimental.pallas import tpu as pltpu
from jax.sharding import PartitionSpec as P

B = 128
NT = 256
EXTRA = 16
VM = pl.BlockSpec(memory_space=pltpu.VMEM)
SM = pl.BlockSpec(memory_space=pltpu.SMEM)
SIN = (6.28318516, -41.34165503, 81.60100407, -76.54978229, 39.53670602)
b = 16


def lane(x, c):
    return jnp.broadcast_to(x[:, c:c + 1], (x.shape[0], B))


def chain(rt, ut, FB):
    rows = lax.broadcasted_iota(jnp.int32, (b, B), 0)
    for p in range(B // b):
        o = p * b
        rd = rt[o:o + b, :B]
        ri = rt[o:o + b, B:]
        C = [lane(rd, o + k) for k in range(b)]
        if o + b < B:
            nd = rt[o + b:o + 2 * b, :B]
            F = [lane(nd, o + k) for k in range(b)]
        RS = []
        for k in range(0, b, 2):
            ca, cb = C[k], C[k + 1]
            pa, pb, pc = ca[k:k + 1, :], ca[k + 1:k + 2, :], cb[k + 1:k + 2, :]
            ra = lax.rsqrt(pa)
            rb = lax.rsqrt(pa * pc - pb * pb) * (pa * ra)
            la = jnp.where(rows == k, 0.0, ca) * ra
            sa = pb * ra
            cb = cb - la * sa
            lb = jnp.where(rows == k + 1, 0.0, cb) * rb
            ua = [x[k:k + 1, :] * ra for x in (rd, ri)]
            ub = [(x[k + 1:k + 2, :] - sa * u) * rb for x, u in zip((rd, ri), ua)]
            ut[o + k:o + k + 1, :B] = ua[0]
            ut[o + k:o + k + 1, B:] = ua[1]
            ut[o + k + 1:o + k + 2, :B] = ub[0]
            ut[o + k + 1:o + k + 2, B:] = ub[1]
            for j in range(k + 2, b):
                ta, tb = la[j:j + 1, :], lb[j:j + 1, :]
                C[j] = (C[j] - la * ta) - lb * tb
            rd = (rd - la * ua[0]) - lb * ub[0]
            ri = (ri - la * ua[1]) - lb * ub[1]
            RS += [ra, rb]
        rv = jnp.concatenate([r * r for r in RS], axis=0)
        if o + b < B:
            rd = rd * rv
            ri = ri * rv
            g = o + b
            xd = rt[g:g + b, :B]
            xi = rt[g:g + b, B:]
            for k in range(b):
                xd = xd - F[k] * rd[k:k + 1, :]
                xi = xi - F[k] * ri[k:k + 1, :]
            rt[g:g + b, :B] = xd
            rt[g:g + b, B:] = xi
        if o + 2 * b < B:
            g = o + 2 * b
            v = split3(jnp.concatenate([rd, ri], axis=1))
            for i, q in enumerate((0, 1, 0, 1, 2, 0)):
                FB[i * B + o:i * B + o + b, :] = v[q]
                if p:
                    FB[i * B + o - b:i * B + o, :] = jnp.zeros((b, 2 * B), jnp.bfloat16)
            f = split3(rt[g:B, :B])
            lhs = jnp.concatenate([f[0], f[0], f[1], f[1], f[0], f[2]], axis=1)
            rt[g:B, :] = rt[g:B, :] - jnp.dot(lhs, FB[...], preferred_element_type=jnp.float32)
    last = B - 3 * b
    for i in range(6):
        FB[i * B + last:i * B + last + b, :] = jnp.zeros((b, 2 * B), jnp.bfloat16)

def split3(x):
    x1 = x.astype(jnp.bfloat16)
    r = x - x1.astype(jnp.float32)
    x2 = r.astype(jnp.bfloat16)
    x3 = (r - x2.astype(jnp.float32)).astype(jnp.bfloat16)
    return x1, x2, x3

def nt(x, y):
    return lax.dot_general(x, y, (((1,), (1,)), ((), ())), preferred_element_type=jnp.float32)

def nt6(x, y):
    l = jnp.concatenate([x[0], x[0], x[1], x[1], x[0], x[2]], axis=1)
    r = jnp.concatenate([y[0], y[1], y[0], y[1], y[2], y[0]], axis=1)
    return nt(l, r)


def extra(ref, which):
    block = ref[ref.shape[0] - EXTRA:, :].astype(jnp.float32)
    at = 3 * which
    return (block[at:at + 1] + block[at + 1:at + 2]) + block[at + 2:at + 3]


def chol_kernel(h_ref, g0, g1, e0, e1, fr, fp, o_ref, rt, ut, L, S1, S2, S3, FB, W, *, n):
    nb = n // B
    half = n // 2
    first = h_ref[0] == 0
    mine_all, other_all = extra(fr, 1), extra(fp, 1)
    ii = lax.broadcasted_iota(jnp.int32, (B, B), 0)
    jj = lax.broadcasted_iota(jnp.int32, (B, B), 1)
    tri = ii >= jj
    eye = (ii == jj).astype(jnp.float32)

    def a(r0, r1, lo):
        if lo < half:
            return g0[r0:r1, lo:lo + B] + e0[r0:r1, lo:lo + B]
        return g1[r0 - half:r1 - half, lo - half:lo - half + B] + e1[r0 - half:r1 - half, lo - half:lo - half + B]

    def ridge_at(lo):
        at = lo % half
        mine, other = mine_all[:, at:at + B], other_all[:, at:at + B]
        row = jnp.where(first, mine, other) if lo < half else jnp.where(first, other, mine)
        return jnp.where(ii == jj, row, 0.0)

    rt[:, :B] = a(0, B, 0) + ridge_at(0)
    FB[...] = jnp.zeros((6 * B, 2 * B), jnp.bfloat16)
    for j in range(nb):
        L[j * B:(j + 1) * B, :] = jnp.zeros((B, n), jnp.float32)

    def step(kk, carry):
        rt[:, B:] = eye
        chain(rt, ut, FB)
        for j in range(nb):
            @pl.when(kk == j)
            def _():
                lo = j * B
                ljj = jnp.where(tri, ut[:, :B].T, 0.0)
                L[lo:lo + B, lo:lo + B] = ljj
                if j + 1 < nb:
                    hi = lo + B
                    ms = split3(jnp.where(tri, ut[:, B:], 0.0))
                    w = W[hi:n, :] if j else a(hi, n, lo)
                    x = nt6(split3(w), ms)
                    L[hi:n, lo:hi] = x
                    S1[hi:n, lo:hi], S2[hi:n, lo:hi], S3[hi:n, lo:hi] = split3(x)
                    w = a(hi, n, hi) - nt6([s[hi:n, 0:hi] for s in (S1, S2, S3)],
                                           [s[hi:hi + B, 0:hi] for s in (S1, S2, S3)])
                    rt[:, :B] = w[:B] + ridge_at(hi)
                    W[hi:n, :] = w
        return carry
    lax.fori_loop(0, nb, step, 0)
    o_ref[...] = L[pl.ds(pl.multiple_of(h_ref[0] * half, half), half), :]


def chol(h, parts, fr, fp):
    n = parts[0].shape[0]
    return pl.pallas_call(
        functools.partial(chol_kernel, n=n),
        out_shape=jax.ShapeDtypeStruct((n // 2, n), jnp.float32),
        in_specs=[SM] + [VM] * 6,
        out_specs=VM,
        scratch_shapes=[pltpu.VMEM((B, 2 * B), jnp.float32), pltpu.VMEM((B, 2 * B), jnp.float32),
                        pltpu.VMEM((n, n), jnp.float32)] + [pltpu.VMEM((n, n), jnp.bfloat16)] * 3
        + [pltpu.VMEM((6 * B, 2 * B), jnp.bfloat16), pltpu.VMEM((n, B), jnp.float32)],
        cost_estimate=pl.CostEstimate(flops=20 * 10**9, bytes_accessed=8 * 2**20, transcendentals=0),
        compiler_params=pltpu.CompilerParams(vmem_limit_bytes=40 * 2**20),
    )(h, *parts, fr, fp)


def feat(pts, wf, turns, scale):
    dot = jnp.dot(pts, wf, preferred_element_type=jnp.float32)
    t = dot * (0.5 / math.pi) + turns
    v = 0.25 - jnp.abs(t - jnp.round(t))
    w = v * v
    poly = w * (scale * SIN[4]) + scale * SIN[3]
    for c in SIN[2::-1]:
        poly = poly * w + scale * c
    return (v * poly).astype(jnp.bfloat16)


def tn(x, y):
    return lax.dot_general(x, y, (((0,), (0,)), ((), ())), preferred_element_type=jnp.float32)


def win_kernel(*refs, nc, acc, scale, rows):
    h_ref, fr, fp = refs[:3]
    din, half = fr.shape[0] - EXTRA, fr.shape[1]
    chunks = refs[3:3 + nc]
    k = 3 + nc
    if acc:
        a0, a1 = refs[k:k + 2]
        k += 2
    g0, g1, own, phi = refs[k:]
    first = h_ref[0] == 0
    tr, tp = extra(fr, 0), extra(fp, 0)
    for i in range(nc):
        pts = chunks[i][:rows, :]
        own[i * rows:(i + 1) * rows, half:] = pts
        own[nc * rows + i * EXTRA:nc * rows + (i + 1) * EXTRA, half:] = chunks[i][rows:, :]
        own[nc * rows + i * EXTRA:nc * rows + (i + 1) * EXTRA, :half] = jnp.zeros((EXTRA, half), jnp.bfloat16)
        for c in range(0, half, NT):
            s = slice(c, c + NT)
            lo = jnp.where(first, fr[:din, s], fp[:din, s])
            hi = jnp.where(first, fp[:din, s], fr[:din, s])
            tlo = jnp.where(first, tr[:, s], tp[:, s])
            thi = jnp.where(first, tp[:, s], tr[:, s])
            phi[i * rows:(i + 1) * rows, c:c + NT] = feat(pts, lo, tlo, scale)
            phi[i * rows:(i + 1) * rows, half + c:half + c + NT] = feat(pts, hi, thi, scale)
    own[:nc * rows, :half] = phi[:, pl.ds(pl.multiple_of(h_ref[0] * half, half), half)]
    for c in range(0, 2 * half, NT):
        lo = 0 if c < half else half
        out, at = (g0, c) if c < half else (g1, c - half)
        r = tn(phi[:, lo:], phi[:, c:c + NT])
        if acc:
            r = r + (a0 if c < half else a1)[:, at:at + NT]
        out[:, at:at + NT] = r


def win(h, fr, fp, chunks, acc, scale, rows):
    din, half = fr.shape[0] - EXTRA, fr.shape[1]
    nc = len(chunks)
    args = [h, fr, fp] + list(chunks) + list(acc or [])
    f32 = jnp.float32
    return pl.pallas_call(
        functools.partial(win_kernel, nc=nc, acc=acc is not None, scale=scale, rows=rows),
        out_shape=[jax.ShapeDtypeStruct((2 * half, half), f32), jax.ShapeDtypeStruct((half, half), f32),
                   jax.ShapeDtypeStruct((nc * (rows + EXTRA), half + din), jnp.bfloat16)],
        in_specs=[SM] + [VM] * (len(args) - 1),
        out_specs=[VM] * 3,
        scratch_shapes=[pltpu.VMEM((nc * rows, 2 * half), jnp.bfloat16)],
        cost_estimate=pl.CostEstimate(flops=nc * rows * 2 * half * (din + 3 * half // 2) * 2,
                                      bytes_accessed=4 * 2**20, transcendentals=0),
        compiler_params=pltpu.CompilerParams(vmem_limit_bytes=32 * 2**20),
    )(*args)


def col_kernel(f_ref, fc, fr, *refs, scale, rows):
    parts = refs[:-3]
    g, pr, phi = refs[-3:]
    din, width = fc.shape[0] - EXTRA, fc.shape[1]
    half = fr.shape[1]
    turns = extra(fc, 0)
    counts = [p.shape[0] // (rows + EXTRA) for p in parts]
    base = 0
    for p, m in zip(parts, counts):
        for i in range(m):
            for c in range(0, width, NT):
                phi[base + i * rows:base + (i + 1) * rows, c:c + NT] = feat(
                    p[i * rows:(i + 1) * rows, half:], fc[:din, c:c + NT], turns[:, c:c + NT], scale)
        base += m * rows
    ii = lax.broadcasted_iota(jnp.int32, (half, NT), 0)
    jj = lax.broadcasted_iota(jnp.int32, (half, NT), 1)
    same = f_ref[0] != 0
    ridge = extra(fr, 1)
    for c in range(0, width, NT):
        total = jnp.where((ii == jj + c) & same, ridge[:, c:c + NT], 0.0)
        base = 0
        for p, m in zip(parts, counts):
            total = total + tn(p[:m * rows, :half], phi[base:base + m * rows, c:c + NT])
            base += m * rows
        g[:, c:c + NT] = total
    total = jnp.zeros((8, half), jnp.float32)
    for p, m in zip(parts, counts):
        t = [p[m * rows + i * EXTRA:m * rows + (i + 1) * EXTRA, half:][:8] for i in range(m)]
        total = total + jnp.dot(jnp.concatenate(t, axis=1), p[:m * rows, :half], preferred_element_type=jnp.float32)
    pr[...] = total


def col(flag, fc, fr, parts, scale, rows):
    width = fc.shape[1]
    half = fr.shape[1]
    args = [flag, fc, fr, *parts]
    total = sum(p.shape[0] // (rows + EXTRA) * rows for p in parts)
    return pl.pallas_call(
        functools.partial(col_kernel, scale=scale, rows=rows),
        out_shape=[jax.ShapeDtypeStruct((half, width), jnp.float32), jax.ShapeDtypeStruct((8, half), jnp.float32)],
        in_specs=[SM] + [VM] * (len(args) - 1),
        out_specs=[VM] * 2,
        scratch_shapes=[pltpu.VMEM((total, width), jnp.bfloat16)],
        cost_estimate=pl.CostEstimate(flops=8 * 10**9, bytes_accessed=12 * 2**20, transcendentals=0),
        compiler_params=pltpu.CompilerParams(vmem_limit_bytes=40 * 2**20),
    )(*args)


def prep_kernel(p, t, f, ph, ri, pack, fpack):
    rows, din = p.shape[0], f.shape[0]
    pack[:rows, :] = p[...]
    pack[rows:, :] = jnp.concatenate([t[...], jnp.zeros_like(t[...])], axis=0)
    fpack[:din, :] = f[...]
    x = list(split3(ph[...] * (0.5 / math.pi))) + list(split3(ri[...]))
    pad = jnp.zeros((EXTRA - 6, f.shape[1]), jnp.float32)
    fpack[din:, :] = jnp.concatenate([v.astype(jnp.float32) for v in x] + [pad], axis=0).astype(jnp.bfloat16)


def prep(points, targets, freqs, phase, ridge):
    rows, din = points.shape
    w = phase.shape[0]
    return pl.pallas_call(
        prep_kernel,
        out_shape=[jax.ShapeDtypeStruct((rows + EXTRA, din), jnp.bfloat16),
                   jax.ShapeDtypeStruct((freqs.shape[0] + EXTRA, w), jnp.bfloat16)],
        in_specs=[VM] * 5,
        out_specs=[VM] * 2,
    )(points, targets, freqs, phase.reshape(1, w), ridge.reshape(1, w))


def shards(points, freqs, phase, ridge, targets):
    nd = lax.axis_size("dp")
    nf = lax.axis_size("feat")
    fi = lax.axis_index("feat")
    di = lax.axis_index("dp")
    nz = nd // 2
    rows = points.shape[0]
    scale = math.sqrt(2.0 / (rows * nd))

    def zshift(x, s):
        return lax.ppermute(x, "dp", [(2 * z + c, 2 * ((z + s) % nz) + c) for z in range(nz) for c in range(2)])

    def sibling(x):
        return lax.ppermute(x, "dp", [(i, i ^ 1) for i in range(nd)])

    def partner(x):
        return lax.ppermute(x, "feat", [(i, i ^ 1) for i in range(nf)])

    def swap(x):
        return lax.ppermute(x, ("dp", "feat"), [(i * nf + j, j * nd + i) for i in range(nd) for j in range(nf)])

    pack, fr = prep(points, targets, freqs, phase, ridge)
    u1, d1, u2, d2 = zshift(pack, 1), zshift(pack, -1), zshift(pack, 2), zshift(pack, -2)
    fp = partner(fr)
    u3, d3, u4 = zshift(u2, 1), zshift(d2, -1), zshift(u2, 2)
    h = jnp.reshape(fi % 2, (1,)).astype(jnp.int32)
    late = lax.optimization_barrier((fr, u2, d2))[0]
    fc = swap(late)
    g0, g1, o1 = win(h, fr, fp, [pack, u1, d1, u2, d2], None, scale, rows)
    s1 = sibling(o1)
    g0, g1, o2 = win(h, fr, fp, [u3, d3, u4], (g0, g1), scale, rows)
    e0, e1 = sibling(g0), sibling(g1)
    s2 = sibling(o2)
    factor_rows = chol(h, (g0, g1, e0, e1), fr, fp)
    flag = jnp.reshape(fi == di, (1,)).astype(jnp.int32)
    flag, factor_rows = lax.optimization_barrier((flag, factor_rows))
    gram_tile, projected = col(flag, fc, fr, (o1, o2, s1, s2), scale, rows)
    return (gram_tile, projected, factor_rows)


def solution(mesh):
    in_specs = (P("dp", None), P(None, "feat"), P("feat"), P("feat"), P(None, "dp"))
    out_specs = (P("feat", "dp"), P(None, "feat"), P("feat", None))
    return jax.shard_map(shards, mesh=mesh, in_specs=in_specs, out_specs=out_specs, check_vma=False)
```

```python
import functools
import math

import jax
import jax.numpy as jnp
from jax import lax
from jax.experimental import pallas as pl
from jax.experimental.pallas import tpu as pltpu
from jax.sharding import PartitionSpec as P

B = 128
NT = 256
EXTRA = 16
VM = pl.BlockSpec(memory_space=pltpu.VMEM)
SM = pl.BlockSpec(memory_space=pltpu.SMEM)
SIN = (6.28316404, -41.33714237, 81.34076887, -70.9934331)
b = 16


def lane(x, c):
    return jnp.broadcast_to(x[:, c:c + 1], (x.shape[0], B))


def chain(rt, ut, FB):
    rows = lax.broadcasted_iota(jnp.int32, (b, B), 0)
    for p in range(B // b):
        o = p * b
        rd = rt[o:o + b, :B]
        ri = rt[o:o + b, B:]
        C = [lane(rd, o + k) for k in range(b)]
        if o + b < B:
            nd = rt[o + b:o + 2 * b, :B]
            F = [lane(nd, o + k) for k in range(b)]
        RS = []
        for k in range(0, b, 2):
            ca, cb = C[k], C[k + 1]
            pa, pb, pc = ca[k:k + 1, :], ca[k + 1:k + 2, :], cb[k + 1:k + 2, :]
            ra = lax.rsqrt(pa)
            rb = lax.rsqrt(pa * pc - pb * pb) * (pa * ra)
            la = jnp.where(rows == k, 0.0, ca) * ra
            sa = pb * ra
            cb = cb - la * sa
            lb = jnp.where(rows == k + 1, 0.0, cb) * rb
            ua = [x[k:k + 1, :] * ra for x in (rd, ri)]
            ub = [(x[k + 1:k + 2, :] - sa * u) * rb for x, u in zip((rd, ri), ua)]
            ut[o + k:o + k + 1, :B] = ua[0]
            ut[o + k:o + k + 1, B:] = ua[1]
            ut[o + k + 1:o + k + 2, :B] = ub[0]
            ut[o + k + 1:o + k + 2, B:] = ub[1]
            for j in range(k + 2, b):
                ta, tb = la[j:j + 1, :], lb[j:j + 1, :]
                C[j] = (C[j] - la * ta) - lb * tb
            rd = (rd - la * ua[0]) - lb * ub[0]
            ri = (ri - la * ua[1]) - lb * ub[1]
            RS += [ra, rb]
        rv = jnp.concatenate([r * r for r in RS], axis=0)
        if o + b < B:
            rd = rd * rv
            ri = ri * rv
            g = o + b
            xd = rt[g:g + b, :B]
            xi = rt[g:g + b, B:]
            for k in range(b):
                xd = xd - F[k] * rd[k:k + 1, :]
                xi = xi - F[k] * ri[k:k + 1, :]
            rt[g:g + b, :B] = xd
            rt[g:g + b, B:] = xi
        if o + 2 * b < B:
            g = o + 2 * b
            v = split3(jnp.concatenate([rd, ri], axis=1))
            for i, q in enumerate((0, 1, 0, 1, 2, 0)):
                FB[i * B + o:i * B + o + b, :] = v[q]
                if p:
                    FB[i * B + o - b:i * B + o, :] = jnp.zeros((b, 2 * B), jnp.bfloat16)
            f = split3(rt[g:B, :B])
            lhs = jnp.concatenate([f[0], f[0], f[1], f[1], f[0], f[2]], axis=1)
            rt[g:B, :] = rt[g:B, :] - jnp.dot(lhs, FB[...], preferred_element_type=jnp.float32)
    last = B - 3 * b
    for i in range(6):
        FB[i * B + last:i * B + last + b, :] = jnp.zeros((b, 2 * B), jnp.bfloat16)

def split3(x):
    x1 = x.astype(jnp.bfloat16)
    r = x - x1.astype(jnp.float32)
    x2 = r.astype(jnp.bfloat16)
    x3 = (r - x2.astype(jnp.float32)).astype(jnp.bfloat16)
    return x1, x2, x3

def nt(x, y):
    return lax.dot_general(x, y, (((1,), (1,)), ((), ())), preferred_element_type=jnp.float32)

def nt6(x, y):
    l = jnp.concatenate([x[0], x[1], x[2], x[0]], axis=1)
    zero = jnp.zeros_like(y[1])
    r = jnp.concatenate([jnp.concatenate([y[0], y[0], y[0], y[2]], axis=1),
                         jnp.concatenate([y[1], y[1], zero, zero], axis=1)], axis=0)
    out = nt(l, r)
    return out[:, :B] + out[:, B:]


def extra(ref, which):
    block = ref[ref.shape[0] - EXTRA:, :].astype(jnp.float32)
    at = 3 * which
    return (block[at:at + 1] + block[at + 1:at + 2]) + block[at + 2:at + 3]


def strip(n, c):
    return c * n - NT * (c * (c - 1) // 2)


def chol_kernel(h_ref, g, e, misc, o_ref, rt, ut, L, S1, S2, S3, FB, W, *, n):
    nb = n // B
    half = n // 2
    ii = lax.broadcasted_iota(jnp.int32, (B, B), 0)
    jj = lax.broadcasted_iota(jnp.int32, (B, B), 1)
    tri = ii >= jj
    eye = (ii == jj).astype(jnp.float32)

    def a(r0, r1, lo):
        c = lo // NT
        at = lo - c * NT
        base = strip(n, c) - c * NT
        return g[base + r0:base + r1, at:at + B] + e[base + r0:base + r1, at:at + B]

    def ridge_at(lo):
        row = misc[0:1, lo:lo + B]
        return jnp.where(ii == jj, row, 0.0)

    rt[:, :B] = a(0, B, 0) + ridge_at(0)
    FB[...] = jnp.zeros((6 * B, 2 * B), jnp.bfloat16)
    for j in range(nb):
        L[j * B:(j + 1) * B, :] = jnp.zeros((B, n), jnp.float32)

    def step(kk, carry):
        rt[:, B:] = eye
        chain(rt, ut, FB)
        for j in range(nb):
            @pl.when(kk == j)
            def _():
                lo = j * B
                ljj = jnp.where(tri, ut[:, :B].T, 0.0)
                L[lo:lo + B, lo:lo + B] = ljj
                if j + 1 < nb:
                    hi = lo + B
                    ms = split3(jnp.where(tri, ut[:, B:], 0.0))
                    w = W[hi:n, :] if j else a(hi, n, lo)
                    x = nt6(split3(w), ms)
                    L[hi:n, lo:hi] = x
                    S1[hi:n, lo:hi], S2[hi:n, lo:hi], S3[hi:n, lo:hi] = split3(x)
                    w = a(hi, n, hi) - nt6([s[hi:n, 0:hi] for s in (S1, S2, S3)],
                                           [s[hi:hi + B, 0:hi] for s in (S1, S2, S3)])
                    rt[:, :B] = w[:B] + ridge_at(hi)
                    W[hi:n, :] = w
        return carry
    lax.fori_loop(0, nb, step, 0)
    o_ref[...] = L[pl.ds(pl.multiple_of(h_ref[0] * half, half), half), :]


def chol(h, g, e, misc):
    n = misc.shape[1]
    return pl.pallas_call(
        functools.partial(chol_kernel, n=n),
        out_shape=jax.ShapeDtypeStruct((n // 2, n), jnp.float32),
        in_specs=[SM] + [VM] * 3,
        out_specs=VM,
        scratch_shapes=[pltpu.VMEM((B, 2 * B), jnp.float32), pltpu.VMEM((B, 2 * B), jnp.float32),
                        pltpu.VMEM((n, n), jnp.float32)] + [pltpu.VMEM((n, n), jnp.bfloat16)] * 3
        + [pltpu.VMEM((6 * B, 2 * B), jnp.bfloat16), pltpu.VMEM((n, B), jnp.float32)],
        cost_estimate=pl.CostEstimate(flops=20 * 10**9, bytes_accessed=8 * 2**20, transcendentals=0),
        compiler_params=pltpu.CompilerParams(vmem_limit_bytes=40 * 2**20),
    )(h, g, e, misc)


def feat(pts, wf, turns, scale):
    dot = jnp.dot(pts, wf, preferred_element_type=jnp.float32)
    t = dot * (0.5 / math.pi) + turns
    v = 0.25 - jnp.abs(t - jnp.round(t))
    w = v * v
    poly = w * (scale * SIN[-1]) + scale * SIN[-2]
    for c in SIN[-3::-1]:
        poly = poly * w + scale * c
    return (v * poly).astype(jnp.bfloat16)


def tn(x, y):
    return lax.dot_general(x, y, (((0,), (0,)), ((), ())), preferred_element_type=jnp.float32)


def win_kernel(*refs, nc, acc, scale, rows):
    h_ref = refs[0]
    if acc:
        wf, misc, a0 = refs[1:4]
        chunks = refs[4:4 + nc]
        out, own, phi = refs[4 + nc:]
        din, full = wf.shape
        half = full // 2
    else:
        fr, fp = refs[1:3]
        chunks = refs[3:3 + nc]
        out, own, wf, misc, phi = refs[3 + nc:]
        din, full = wf.shape
        half = full // 2
        first = h_ref[0] == 0
        wf[:, :half] = jnp.where(first, fr[:din, :], fp[:din, :])
        wf[:, half:] = jnp.where(first, fp[:din, :], fr[:din, :])
        for which, at in ((1, 0), (0, 8)):
            mine, other = extra(fr, which), extra(fp, which)
            row = jnp.concatenate([jnp.where(first, mine, other), jnp.where(first, other, mine)], axis=1)
            misc[at:at + 1, :] = row
        misc[1:2, :half] = extra(fr, 1)
        misc[1:2, half:] = extra(fp, 1)
    turns = misc[8:9, :]
    for i in range(nc):
        pts = chunks[i][:rows, :]
        own[i * rows:(i + 1) * rows, half:] = pts
        own[nc * rows + i * EXTRA:nc * rows + (i + 1) * EXTRA, half:] = chunks[i][rows:, :]
        own[nc * rows + i * EXTRA:nc * rows + (i + 1) * EXTRA, :half] = jnp.zeros((EXTRA, half), jnp.bfloat16)
        for c in range(0, full, NT):
            phi[i * rows:(i + 1) * rows, c:c + NT] = feat(pts, wf[:, c:c + NT], turns[:, c:c + NT], scale)
    own[:nc * rows, :half] = phi[:, pl.ds(pl.multiple_of(h_ref[0] * half, half), half)]
    for c in range(full // NT):
        at = strip(full, c)
        r = tn(phi[:, c * NT:], phi[:, c * NT:(c + 1) * NT])
        if acc:
            r = r + a0[at:at + r.shape[0], :]
        out[at:at + r.shape[0], :] = r


def win(h, weights, chunks, before, scale, rows):
    acc = before is not None
    f32, bf = jnp.float32, jnp.bfloat16
    if acc:
        din, full = weights[0].shape
    else:
        din, full = weights[0].shape[0] - EXTRA, 2 * weights[0].shape[1]
    nc = len(chunks)
    args = [h, *weights] + ([before] if acc else []) + list(chunks)
    shapes = [((strip(full, full // NT), NT), f32), ((nc * (rows + EXTRA), full // 2 + din), bf)]
    if not acc:
        shapes += [((din, full), bf), ((16, full), f32)]
    return pl.pallas_call(
        functools.partial(win_kernel, nc=nc, acc=acc, scale=scale, rows=rows),
        out_shape=[pltpu.VMEM(s, d) for s, d in shapes],
        in_specs=[SM] + [VM] * (len(args) - 1),
        out_specs=[VM] * len(shapes),
        scratch_shapes=[pltpu.VMEM((nc * rows, full), bf)],
        cost_estimate=pl.CostEstimate(flops=nc * rows * full * (din + full * 5 // 8) * 2,
                                      bytes_accessed=4 * 2**20, transcendentals=0),
        compiler_params=pltpu.CompilerParams(vmem_limit_bytes=32 * 2**20),
    )(*args)


def col_kernel(f_ref, fc, misc, *refs, scale, rows):
    parts = refs[:-3]
    g, pr, phi = refs[-3:]
    din, width = fc.shape[0] - EXTRA, fc.shape[1]
    half = misc.shape[1] // 2
    turns = extra(fc, 0)
    counts = [p.shape[0] // (rows + EXTRA) for p in parts]
    base = 0
    for p, m in zip(parts, counts):
        for i in range(m):
            for c in range(0, width, NT):
                phi[base + i * rows:base + (i + 1) * rows, c:c + NT] = feat(
                    p[i * rows:(i + 1) * rows, half:], fc[:din, c:c + NT], turns[:, c:c + NT], scale)
        base += m * rows
    ii = lax.broadcasted_iota(jnp.int32, (half, NT), 0)
    jj = lax.broadcasted_iota(jnp.int32, (half, NT), 1)
    same = f_ref[0] != 0
    ridge = misc[1:2, :half]
    for c in range(0, width, NT):
        total = jnp.where((ii == jj + c) & same, ridge[:, c:c + NT], 0.0)
        base = 0
        for p, m in zip(parts, counts):
            total = total + tn(p[:m * rows, :half], phi[base:base + m * rows, c:c + NT])
            base += m * rows
        g[:, c:c + NT] = total
    total = jnp.zeros((8, half), jnp.float32)
    for p, m in zip(parts, counts):
        t = [p[m * rows + i * EXTRA:m * rows + (i + 1) * EXTRA, half:][:8] for i in range(m)]
        total = total + jnp.dot(jnp.concatenate(t, axis=1), p[:m * rows, :half], preferred_element_type=jnp.float32)
    pr[...] = total


def col(flag, fc, misc, parts, scale, rows):
    width = fc.shape[1]
    half = misc.shape[1] // 2
    args = [flag, fc, misc, *parts]
    total = sum(p.shape[0] // (rows + EXTRA) * rows for p in parts)
    return pl.pallas_call(
        functools.partial(col_kernel, scale=scale, rows=rows),
        out_shape=[jax.ShapeDtypeStruct((half, width), jnp.float32), jax.ShapeDtypeStruct((8, half), jnp.float32)],
        in_specs=[SM] + [VM] * (len(args) - 1),
        out_specs=[VM] * 2,
        scratch_shapes=[pltpu.VMEM((total, width), jnp.bfloat16)],
        cost_estimate=pl.CostEstimate(flops=8 * 10**9, bytes_accessed=12 * 2**20, transcendentals=0),
        compiler_params=pltpu.CompilerParams(vmem_limit_bytes=40 * 2**20),
    )(*args)


def prep_kernel(p, t, f, ph, ri, pack, fpack):
    rows, din = p.shape[0], f.shape[0]
    pack[:rows, :] = p[...]
    pack[rows:, :] = jnp.concatenate([t[...], jnp.zeros_like(t[...])], axis=0)
    fpack[:din, :] = f[...]
    x = list(split3(ph[...] * (0.5 / math.pi))) + list(split3(ri[...]))
    pad = jnp.zeros((EXTRA - 6, f.shape[1]), jnp.float32)
    fpack[din:, :] = jnp.concatenate([v.astype(jnp.float32) for v in x] + [pad], axis=0).astype(jnp.bfloat16)


def prep(points, targets, freqs, phase, ridge):
    rows, din = points.shape
    w = phase.shape[0]
    return pl.pallas_call(
        prep_kernel,
        out_shape=[pltpu.VMEM((rows + EXTRA, din), jnp.bfloat16),
                   pltpu.VMEM((freqs.shape[0] + EXTRA, w), jnp.bfloat16)],
        in_specs=[VM] * 5,
        out_specs=[VM] * 2,
    )(points, targets, freqs, phase.reshape(1, w), ridge.reshape(1, w))


def shards(points, freqs, phase, ridge, targets):
    nd = lax.axis_size("dp")
    nf = lax.axis_size("feat")
    fi = lax.axis_index("feat")
    di = lax.axis_index("dp")
    nz = nd // 2
    rows = points.shape[0]
    scale = math.sqrt(2.0 / (rows * nd))

    def zshift(x, s):
        return lax.ppermute(x, "dp", [(2 * z + c, 2 * ((z + s) % nz) + c) for z in range(nz) for c in range(2)])

    def sibling(x):
        return lax.ppermute(x, "dp", [(i, i ^ 1) for i in range(nd)])

    def partner(x):
        return lax.ppermute(x, "feat", [(i, i ^ 1) for i in range(nf)])

    def swap(x):
        return lax.ppermute(x, ("dp", "feat"), [(i * nf + j, j * nd + i) for i in range(nd) for j in range(nf)])

    pack, fr = prep(points, targets, freqs, phase, ridge)
    u1, d1, u2, d2 = zshift(pack, 1), zshift(pack, -1), zshift(pack, 2), zshift(pack, -2)
    fp = partner(fr)
    u3, d3, u4 = zshift(u2, 1), zshift(d2, -1), zshift(u2, 2)
    h = jnp.reshape(fi % 2, (1,)).astype(jnp.int32)
    late = lax.optimization_barrier((fr, u2, d2))[0]
    fc = swap(late)
    g, o1, wf, misc = win(h, (fr, fp), [pack, u1, d1, u2, d2], None, scale, rows)
    s1 = sibling(o1)
    g, o2 = win(h, (wf, misc), [u3, d3, u4], g, scale, rows)
    e = sibling(g)
    s2 = sibling(o2)
    factor_rows = chol(h, g, e, misc)
    flag = jnp.reshape(fi == di, (1,)).astype(jnp.int32)
    flag, factor_rows = lax.optimization_barrier((flag, factor_rows))
    gram_tile, projected = col(flag, fc, misc, (o1, o2, s1, s2), scale, rows)
    return (gram_tile, projected, factor_rows)


def solution(mesh):
    in_specs = (P("dp", None), P(None, "feat"), P("feat"), P("feat"), P(None, "dp"))
    out_specs = (P("feat", "dp"), P(None, "feat"), P("feat", None))
    return jax.shard_map(shards, mesh=mesh, in_specs=in_specs, out_specs=out_specs, check_vma=False)
```

```python
import functools
import math

import jax
import jax.numpy as jnp
from jax import lax
from jax.experimental import pallas as pl
from jax.experimental.pallas import tpu as pltpu
from jax.sharding import PartitionSpec as P

B = 128
NT = 256
EXTRA = 16
VM = pl.BlockSpec(memory_space=pltpu.VMEM)
SM = pl.BlockSpec(memory_space=pltpu.SMEM)
HB = pl.BlockSpec(memory_space=pltpu.HBM)
DMA = pltpu.SemaphoreType.DMA
SIN = (6.28316404, -41.33714237, 81.34076887, -70.9934331)
b = 16


def lane(x, c):
    return jnp.broadcast_to(x[:, c:c + 1], (x.shape[0], B))


def chain(rt, ut, FB, LD):
    rows = lax.broadcasted_iota(jnp.int32, (b, B), 0)
    lanes = lax.broadcasted_iota(jnp.int32, (b, B), 1)
    for p in range(B // b):
        o = p * b
        rd = rt[o:o + b, :]
        C = [lane(rd, o + k) for k in range(b)]
        inside = (lanes >= o) & (lanes < o + b)
        rd = jnp.where(inside, jnp.where(lanes == rows + o, 1.0, 0.0), rd)
        if o + b < B:
            xd = rt[o + b:o + 2 * b, :]
            F = [lane(xd, o + k) for k in range(b)]
            xd = jnp.where(inside, 0.0, xd)
        RS, DG = [], []
        ld = jnp.zeros((b, B), jnp.float32)
        for k in range(0, b, 2):
            ca, cb = C[k], C[k + 1]
            pa, pb, pc = ca[k:k + 1, :], ca[k + 1:k + 2, :], cb[k + 1:k + 2, :]
            ra = lax.rsqrt(pa)
            det = pa * pc - pb * pb
            rb = lax.rsqrt(det) * (pa * ra)
            la = jnp.where(rows == k, 0.0, ca) * ra
            sa = pb * ra
            cb = cb - la * sa
            lb = jnp.where(rows == k + 1, 0.0, cb) * rb
            ua = rd[k:k + 1, :] * ra
            ub = (rd[k + 1:k + 2, :] - sa * ua) * rb
            ut[o + k:o + k + 1, :] = ua
            ut[o + k + 1:o + k + 2, :] = ub
            for j in range(k + 2, b):
                ta, tb = la[j:j + 1, :], lb[j:j + 1, :]
                C[j] = (C[j] - la * ta) - lb * tb
            rd = (rd - la * ua) - lb * ub
            ld = jnp.where(lanes == o + k, la, jnp.where(lanes == o + k + 1, lb, ld))
            RS += [ra, rb]
            DG += [pa * ra, cb[k + 1:k + 2, :] * rb]
        LD[o:o + b, :] = jnp.where(lanes < rows + o, ld, jnp.where(lanes == rows + o, jnp.concatenate(DG, axis=0), 0.0))
        if o + b < B:
            rv = jnp.concatenate([r * r for r in RS], axis=0)
            rd = rd * rv
            for k in range(b):
                xd = xd - F[k] * rd[k:k + 1, :]
        if o + 2 * b < B:
            g = o + 2 * b
            v = split3(rd)
            for i, q in enumerate((0, 0, 0, 2)):
                FB[i * B + o:i * B + o + b, :B] = v[q]
                if i < 2:
                    FB[i * B + o:i * B + o + b, B:] = v[1]
                if p:
                    FB[i * B + o - b:i * B + o, :] = jnp.zeros((b, 2 * B), jnp.bfloat16)
            x = rt[g:B, :]
            f = split3(x)
            lhs = jnp.concatenate([f[0], f[1], f[2], f[0]], axis=1)
            far = lax.broadcasted_iota(jnp.int32, (B - g, B), 1)
            d = jnp.dot(lhs, FB[...], preferred_element_type=jnp.float32)
            rt[g:B, :] = (jnp.where((far >= o) & (far < o + b), 0.0, x) - d[:, :B]) - d[:, B:]
        if o + b < B:
            rt[o + b:o + 2 * b, :] = xd
    last = B - 3 * b
    for i in range(4):
        FB[i * B + last:i * B + last + b, :] = jnp.zeros((b, 2 * B), jnp.bfloat16)


def split3(x):
    x1 = x.astype(jnp.bfloat16)
    r = x - x1.astype(jnp.float32)
    x2 = r.astype(jnp.bfloat16)
    x3 = (r - x2.astype(jnp.float32)).astype(jnp.bfloat16)
    return x1, x2, x3


def nt(x, y):
    return lax.dot_general(x, y, (((1,), (1,)), ((), ())), preferred_element_type=jnp.float32)


def nt6(x, y):
    l = jnp.concatenate([x[0], x[1], x[2], x[0]], axis=1)
    zero = jnp.zeros_like(y[1])
    r = jnp.concatenate([jnp.concatenate([y[0], y[0], y[0], y[2]], axis=1),
                         jnp.concatenate([y[1], y[1], zero, zero], axis=1)], axis=0)
    out = nt(l, r)
    return out[:, :B] + out[:, B:]


def extra(ref, which):
    block = ref[ref.shape[0] - EXTRA:, :].astype(jnp.float32)
    at = 3 * which
    return (block[at:at + 1] + block[at + 1:at + 2]) + block[at + 2:at + 3]


def strip(n, c):
    return c * n - NT * (c * (c - 1) // 2)


def chol_kernel(h_ref, g, e, misc, o_ref, rt, ut, L, S1, S2, S3, FB, W, LD, sems, *, n):
    nb = n // B
    half = n // 2
    ii = lax.broadcasted_iota(jnp.int32, (B, B), 0)
    jj = lax.broadcasted_iota(jnp.int32, (B, B), 1)
    tri = ii >= jj
    right = jj >= (ii // b + 1) * b
    row0 = pl.multiple_of(h_ref[0] * half, half)

    def leave(j):
        return pltpu.make_async_copy(L.at[pl.ds(row0, half), pl.ds(j * B, B)], o_ref.at[:, pl.ds(j * B, B)], sems.at[j])


    def a(r0, r1, lo):
        c = lo // NT
        at = lo - c * NT
        base = strip(n, c) - c * NT
        return g[base + r0:base + r1, at:at + B] + e[base + r0:base + r1, at:at + B]

    def ridge_at(lo):
        row = misc[0:1, lo:lo + B]
        return jnp.where(ii == jj, row, 0.0)

    rt[...] = a(0, B, 0) + ridge_at(0)
    FB[...] = jnp.zeros((4 * B, 2 * B), jnp.bfloat16)
    for j in range(nb):
        L[j * B:(j + 1) * B, :] = jnp.zeros((B, n), jnp.float32)

    def step(kk, carry):
        chain(rt, ut, FB, LD)
        for j in range(nb):
            @pl.when(kk == j)
            def _():
                lo = j * B
                if j:
                    leave(j - 1).start()
                ljj = jnp.where(right, ut[...], 0.0).T + LD[...]
                L[lo:lo + B, lo:lo + B] = ljj
                if j + 1 < nb:
                    hi = lo + B
                    ms = split3(jnp.where(tri, ut[...], 0.0))
                    w = W[hi:n, :] if j else a(hi, n, lo)
                    x = nt6(split3(w), ms)
                    L[hi:n, lo:hi] = x
                    S1[hi:n, lo:hi], S2[hi:n, lo:hi], S3[hi:n, lo:hi] = split3(x)
                    w = a(hi, n, hi) - nt6([s[hi:n, 0:hi] for s in (S1, S2, S3)],
                                           [s[hi:hi + B, 0:hi] for s in (S1, S2, S3)])
                    rt[...] = w[:B] + ridge_at(hi)
                    W[hi:n, :] = w
        return carry
    lax.fori_loop(0, nb, step, 0)
    for j in range(nb - 1):
        leave(j).wait()
    leave(nb - 1).start()
    leave(nb - 1).wait()


def chol(h, g, e, misc):
    n = misc.shape[1]
    return pl.pallas_call(
        functools.partial(chol_kernel, n=n),
        out_shape=pltpu.HBM((n // 2, n), jnp.float32),
        in_specs=[SM] + [VM] * 3,
        out_specs=HB,
        scratch_shapes=[pltpu.VMEM((B, B), jnp.float32), pltpu.VMEM((B, B), jnp.float32),
                        pltpu.VMEM((n, n), jnp.float32)] + [pltpu.VMEM((n, n), jnp.bfloat16)] * 3
        + [pltpu.VMEM((4 * B, 2 * B), jnp.bfloat16), pltpu.VMEM((n, B), jnp.float32), pltpu.VMEM((B, B), jnp.float32), DMA((n // B,))],
        cost_estimate=pl.CostEstimate(flops=10**9, bytes_accessed=8 * 2**20, transcendentals=0),
        compiler_params=pltpu.CompilerParams(vmem_limit_bytes=24 * 2**20),
    )(h, g, e, misc)


def feat(pts, wf, turns, scale):
    dot = jnp.dot(pts, wf, preferred_element_type=jnp.float32)
    t = dot * (0.5 / math.pi) + turns
    v = 0.25 - jnp.abs(t - jnp.round(t))
    w = v * v
    poly = w * (scale * SIN[-1]) + scale * SIN[-2]
    for c in SIN[-3::-1]:
        poly = poly * w + scale * c
    return (v * poly).astype(jnp.bfloat16)


def tn(x, y):
    return lax.dot_general(x, y, (((0,), (0,)), ((), ())), preferred_element_type=jnp.float32)


def win_kernel(*refs, nc, acc, scale, rows):
    h_ref = refs[0]
    if acc:
        wf, misc, a0 = refs[1:4]
        chunks = refs[4:4 + nc]
        out, far, phi, sems = refs[4 + nc:]
        din, full = wf.shape
        half = full // 2
    else:
        fr, fp = refs[1:3]
        chunks = refs[3:3 + nc]
        out, far, wf, misc, phi, sems = refs[3 + nc:]
        din, full = wf.shape
        half = full // 2
        first = h_ref[0] == 0
        wf[:, :half] = jnp.where(first, fr[:din, :], fp[:din, :])
        wf[:, half:] = jnp.where(first, fp[:din, :], fr[:din, :])
        for which, at in ((1, 0), (0, 8)):
            mine, other = extra(fr, which), extra(fp, which)
            row = jnp.concatenate([jnp.where(first, mine, other), jnp.where(first, other, mine)], axis=1)
            misc[at:at + 1, :] = row
        misc[1:2, :half] = extra(fr, 1)
        misc[1:2, half:] = extra(fp, 1)
    turns = misc[8:9, :]
    col0 = pl.multiple_of(h_ref[0] * half, half)

    def leave(i, what):
        at = pl.ds(i * rows, rows)
        last = pl.ds(nc * rows + i * EXTRA, EXTRA)
        src, dst = (
            (chunks[i].at[pl.ds(0, rows), :], far.at[at, pl.ds(half, din)]),
            (chunks[i].at[pl.ds(rows, EXTRA), :], far.at[last, pl.ds(half, din)]),
            (phi.at[at, pl.ds(col0, half)], far.at[at, pl.ds(0, half)]),
        )[what]
        return pltpu.make_async_copy(src, dst, sems.at[i, what])

    for i in range(nc):
        leave(i, 0).start()
        leave(i, 1).start()
    for i in range(nc):
        pts = chunks[i][:rows, :]
        for c in range(0, full, NT):
            phi[i * rows:(i + 1) * rows, c:c + NT] = feat(pts, wf[:, c:c + NT], turns[:, c:c + NT], scale)
        if i:
            leave(i - 1, 2).start()
    for c in range(full // NT):
        at = strip(full, c)
        r = tn(phi[:, c * NT:], phi[:, c * NT:(c + 1) * NT])
        if acc:
            r = r + a0[at:at + r.shape[0], :]
        out[at:at + r.shape[0], :] = r
        if c == 0:
            leave(nc - 1, 2).start()
    for i in range(nc):
        for what in range(3):
            leave(i, what).wait()


def win(h, weights, chunks, before, scale, rows):
    acc = before is not None
    f32, bf = jnp.float32, jnp.bfloat16
    if acc:
        din, full = weights[0].shape
    else:
        din, full = weights[0].shape[0] - EXTRA, 2 * weights[0].shape[1]
    nc = len(chunks)
    args = [h, *weights] + ([before] if acc else []) + list(chunks)
    shapes = [((strip(full, full // NT), NT), f32), ((nc * (rows + EXTRA), full // 2 + din), bf)]
    if not acc:
        shapes += [((din, full), bf), ((16, full), f32)]
    return pl.pallas_call(
        functools.partial(win_kernel, nc=nc, acc=acc, scale=scale, rows=rows),
        out_shape=[(pltpu.HBM if i == 1 else pltpu.VMEM)(s, d) for i, (s, d) in enumerate(shapes)],
        in_specs=[SM] + [VM] * (len(args) - 1),
        out_specs=[HB if i == 1 else VM for i in range(len(shapes))],
        scratch_shapes=[pltpu.VMEM((nc * rows, full), bf), DMA((nc, 3))],
        cost_estimate=pl.CostEstimate(flops=nc * rows * full * (din + full * 5 // 8) * 2,
                                      bytes_accessed=4 * 2**20, transcendentals=0),
        compiler_params=pltpu.CompilerParams(vmem_limit_bytes=20 * 2**20),
    )(*args)


def col_kernel(f_ref, fc, misc, *refs, scale, rows):
    n = (len(refs) - 4) // 2
    g, pr, phi = refs[n:n + 3]
    parts, sems = refs[n + 3:-1], refs[-1]
    copies = [pltpu.make_async_copy(refs[i], parts[i], sems.at[i]) for i in range(n)]
    for copy in copies:
        copy.start()
    din, width = fc.shape[0] - EXTRA, fc.shape[1]
    half = misc.shape[1] // 2
    turns = extra(fc, 0)
    counts = [p.shape[0] // (rows + EXTRA) for p in parts]
    base = 0
    for copy, p, m in zip(copies, parts, counts):
        copy.wait()
        for i in range(m):
            for c in range(0, width, NT):
                phi[base + i * rows:base + (i + 1) * rows, c:c + NT] = feat(
                    p[i * rows:(i + 1) * rows, half:], fc[:din, c:c + NT], turns[:, c:c + NT], scale)
        base += m * rows
    ii = lax.broadcasted_iota(jnp.int32, (half, NT), 0)
    jj = lax.broadcasted_iota(jnp.int32, (half, NT), 1)
    same = f_ref[0] != 0
    ridge = misc[1:2, :half]
    for c in range(0, width, NT):
        total = jnp.where((ii == jj + c) & same, ridge[:, c:c + NT], 0.0)
        base = 0
        for p, m in zip(parts, counts):
            total = total + tn(p[:m * rows, :half], phi[base:base + m * rows, c:c + NT])
            base += m * rows
        g[:, c:c + NT] = total
    total = jnp.zeros((8, half), jnp.float32)
    for p, m in zip(parts, counts):
        t = [p[m * rows + i * EXTRA:m * rows + (i + 1) * EXTRA, half:][:8] for i in range(m)]
        total = total + jnp.dot(jnp.concatenate(t, axis=1), p[:m * rows, :half], preferred_element_type=jnp.float32)
    pr[...] = total


def col(flag, fc, misc, parts, scale, rows):
    width = fc.shape[1]
    half = misc.shape[1] // 2
    args = [flag, fc, misc, *parts]
    total = sum(p.shape[0] // (rows + EXTRA) * rows for p in parts)
    return pl.pallas_call(
        functools.partial(col_kernel, scale=scale, rows=rows),
        out_shape=[jax.ShapeDtypeStruct((half, width), jnp.float32), jax.ShapeDtypeStruct((8, half), jnp.float32)],
        in_specs=[SM, VM, VM] + [HB] * len(parts),
        out_specs=[VM] * 2,
        scratch_shapes=[pltpu.VMEM((total, width), jnp.bfloat16)]
        + [pltpu.VMEM(p.shape, p.dtype) for p in parts] + [DMA((len(parts),))],
        cost_estimate=pl.CostEstimate(flops=8 * 10**9, bytes_accessed=12 * 2**20, transcendentals=0),
        compiler_params=pltpu.CompilerParams(vmem_limit_bytes=24 * 2**20),
    )(*args)


def prep_kernel(p, t, f, ph, ri, pack, fpack):
    rows, din = p.shape[0], f.shape[0]
    pack[:rows, :] = p[...]
    pack[rows:, :] = jnp.concatenate([t[...], jnp.zeros_like(t[...])], axis=0)
    fpack[:din, :] = f[...]
    x = list(split3(ph[...] * (0.5 / math.pi))) + list(split3(ri[...]))
    pad = jnp.zeros((EXTRA - 6, f.shape[1]), jnp.float32)
    fpack[din:, :] = jnp.concatenate([v.astype(jnp.float32) for v in x] + [pad], axis=0).astype(jnp.bfloat16)


def prep(points, targets, freqs, phase, ridge):
    rows, din = points.shape
    w = phase.shape[0]
    return pl.pallas_call(
        prep_kernel,
        out_shape=[pltpu.VMEM((rows + EXTRA, din), jnp.bfloat16),
                   pltpu.VMEM((freqs.shape[0] + EXTRA, w), jnp.bfloat16)],
        in_specs=[VM] * 5,
        out_specs=[VM] * 2,
    )(points, targets, freqs, phase.reshape(1, w), ridge.reshape(1, w))


def shards(points, freqs, phase, ridge, targets):
    nd = lax.axis_size("dp")
    nf = lax.axis_size("feat")
    fi = lax.axis_index("feat")
    di = lax.axis_index("dp")
    nz = nd // 2
    rows = points.shape[0]
    scale = math.sqrt(2.0 / (rows * nd))

    def zshift(x, s):
        return lax.ppermute(x, "dp", [(2 * z + c, 2 * ((z + s) % nz) + c) for z in range(nz) for c in range(2)])

    def sibling(x):
        return lax.ppermute(x, "dp", [(i, i ^ 1) for i in range(nd)])

    def partner(x):
        return lax.ppermute(x, "feat", [(i, i ^ 1) for i in range(nf)])

    def swap(x):
        return lax.ppermute(x, ("dp", "feat"), [(i * nf + j, j * nd + i) for i in range(nd) for j in range(nf)])

    pack, fr = prep(points, targets, freqs, phase, ridge)
    u1, d1, u2, d2 = zshift(pack, 1), zshift(pack, -1), zshift(pack, 2), zshift(pack, -2)
    fp = partner(fr)
    u3, d3, u4 = zshift(u2, 1), zshift(d2, -1), zshift(u2, 2)
    h = jnp.reshape(fi % 2, (1,)).astype(jnp.int32)
    late = lax.optimization_barrier((fr, u2, d2))[0]
    fc = swap(late)
    g, o1, wf, misc = win(h, (fr, fp), [pack, u1, d1, u2, d2], None, scale, rows)
    s1 = sibling(o1)
    g, o2 = win(h, (wf, misc), [u3, d3, u4], g, scale, rows)
    e = sibling(g)
    s2 = sibling(o2)
    factor_rows = chol(h, g, e, misc)
    flag = jnp.reshape(fi == di, (1,)).astype(jnp.int32)
    flag, factor_rows = lax.optimization_barrier((flag, factor_rows))
    gram_tile, projected = col(flag, fc, misc, (o1, o2, s1, s2), scale, rows)
    return (gram_tile, projected, factor_rows)


def solution(mesh):
    in_specs = (P("dp", None), P(None, "feat"), P("feat"), P("feat"), P(None, "dp"))
    out_specs = (P("feat", "dp"), P(None, "feat"), P("feat", None))
    return jax.shard_map(shards, mesh=mesh, in_specs=in_specs, out_specs=out_specs, check_vma=False)
```

```python
import functools
import math

import jax
import jax.numpy as jnp
from jax import lax
from jax.experimental import pallas as pl
from jax.experimental.pallas import tpu as pltpu
from jax.sharding import PartitionSpec as P

B = 128
NT = 256
EXTRA = 16
VM = pl.BlockSpec(memory_space=pltpu.VMEM)
SM = pl.BlockSpec(memory_space=pltpu.SMEM)
HB = pl.BlockSpec(memory_space=pltpu.HBM)
DMA = pltpu.SemaphoreType.DMA
SIN = (6.28316404, -41.33714237, 81.34076887, -70.9934331)
b = 16


def lane(x, c):
    return jnp.broadcast_to(x[:, c:c + 1], (x.shape[0], B))


def chain(rt, ut, FB, LD):
    rows = lax.broadcasted_iota(jnp.int32, (b, B), 0)
    lanes = lax.broadcasted_iota(jnp.int32, (b, B), 1)
    for p in range(B // b):
        o = p * b
        rd = rt[o:o + b, :]
        C = [lane(rd, o + k) for k in range(b)]
        inside = (lanes >= o) & (lanes < o + b)
        rd = jnp.where(inside, jnp.where(lanes == rows + o, 1.0, 0.0), rd)
        if o + b < B:
            xd = rt[o + b:o + 2 * b, :]
            F = [lane(xd, o + k) for k in range(b)]
            xd = jnp.where(inside, 0.0, xd)
        RS, DG = [], []
        ld = jnp.zeros((b, B), jnp.float32)
        for k in range(0, b, 2):
            ca, cb = C[k], C[k + 1]
            pa, pb, pc = ca[k:k + 1, :], ca[k + 1:k + 2, :], cb[k + 1:k + 2, :]
            ra = lax.rsqrt(pa)
            det = pa * pc - pb * pb
            rb = lax.rsqrt(det) * (pa * ra)
            la = jnp.where(rows == k, 0.0, ca) * ra
            sa = pb * ra
            cb = cb - la * sa
            lb = jnp.where(rows == k + 1, 0.0, cb) * rb
            ua = rd[k:k + 1, :] * ra
            ub = (rd[k + 1:k + 2, :] - sa * ua) * rb
            ut[o + k:o + k + 1, :] = ua
            ut[o + k + 1:o + k + 2, :] = ub
            for j in range(k + 2, b):
                ta, tb = la[j:j + 1, :], lb[j:j + 1, :]
                C[j] = (C[j] - la * ta) - lb * tb
            rd = (rd - la * ua) - lb * ub
            ld = jnp.where(lanes == o + k, la, jnp.where(lanes == o + k + 1, lb, ld))
            RS += [ra, rb]
            DG += [pa * ra, cb[k + 1:k + 2, :] * rb]
        LD[o:o + b, :] = jnp.where(lanes < rows + o, ld, jnp.where(lanes == rows + o, jnp.concatenate(DG, axis=0), 0.0))
        if o + b < B:
            rv = jnp.concatenate([r * r for r in RS], axis=0)
            rd = rd * rv
            for k in range(b):
                xd = xd - F[k] * rd[k:k + 1, :]
        if o + 2 * b < B:
            g = o + 2 * b
            v = split3(rd)
            for i, q in enumerate((0, 0, 0, 2)):
                FB[i * B + o:i * B + o + b, :B] = v[q]
                if i < 2:
                    FB[i * B + o:i * B + o + b, B:] = v[1]
                if p:
                    FB[i * B + o - b:i * B + o, :] = jnp.zeros((b, 2 * B), jnp.bfloat16)
            x = rt[g:B, :]
            f = split3(x)
            lhs = jnp.concatenate([f[0], f[1], f[2], f[0]], axis=1)
            far = lax.broadcasted_iota(jnp.int32, (B - g, B), 1)
            d = jnp.dot(lhs, FB[...], preferred_element_type=jnp.float32)
            rt[g:B, :] = (jnp.where((far >= o) & (far < o + b), 0.0, x) - d[:, :B]) - d[:, B:]
        if o + b < B:
            rt[o + b:o + 2 * b, :] = xd
    last = B - 3 * b
    for i in range(4):
        FB[i * B + last:i * B + last + b, :] = jnp.zeros((b, 2 * B), jnp.bfloat16)


def split3(x):
    x1 = x.astype(jnp.bfloat16)
    r = x - x1.astype(jnp.float32)
    x2 = r.astype(jnp.bfloat16)
    x3 = (r - x2.astype(jnp.float32)).astype(jnp.bfloat16)
    return x1, x2, x3


def nt(x, y):
    return lax.dot_general(x, y, (((1,), (1,)), ((), ())), preferred_element_type=jnp.float32)


def nt6(x, y):
    l = jnp.concatenate([x[0], x[1], x[2], x[0]], axis=1)
    zero = jnp.zeros_like(y[1])
    r = jnp.concatenate([jnp.concatenate([y[0], y[0], y[0], y[2]], axis=1),
                         jnp.concatenate([y[1], y[1], zero, zero], axis=1)], axis=0)
    out = nt(l, r)
    return out[:, :B] + out[:, B:]


def extra(ref, which):
    block = ref[ref.shape[0] - EXTRA:, :].astype(jnp.float32)
    at = 3 * which
    return (block[at:at + 1] + block[at + 1:at + 2]) + block[at + 2:at + 3]


def strip(n, c):
    return c * n - NT * (c * (c - 1) // 2)


def chol_kernel(h_ref, g, e, misc, o_ref, rt, ut, L, S1, S2, S3, FB, W, LD, sems, *, n):
    nb = n // B
    half = n // 2
    ii = lax.broadcasted_iota(jnp.int32, (B, B), 0)
    jj = lax.broadcasted_iota(jnp.int32, (B, B), 1)
    tri = ii >= jj
    right = jj >= (ii // b + 1) * b
    row0 = pl.multiple_of(h_ref[0] * half, half)

    def leave(j):
        return pltpu.make_async_copy(L.at[pl.ds(row0, half), pl.ds(j * B, B)], o_ref.at[:, pl.ds(j * B, B)], sems.at[j])


    def a(r0, r1, lo):
        c = lo // NT
        at = lo - c * NT
        base = strip(n, c) - c * NT
        return g[base + r0:base + r1, at:at + B] + e[base + r0:base + r1, at:at + B]

    def ridge_at(lo):
        row = misc[0:1, lo:lo + B]
        return jnp.where(ii == jj, row, 0.0)

    rt[...] = a(0, B, 0) + ridge_at(0)
    FB[...] = jnp.zeros((4 * B, 2 * B), jnp.bfloat16)
    for j in range(nb - 1):
        L[j * B:(j + 1) * B, (j + 1) * B:] = jnp.zeros((B, n - (j + 1) * B), jnp.float32)

    def step(kk, carry):
        chain(rt, ut, FB, LD)
        for j in range(nb):
            @pl.when(kk == j)
            def _():
                lo = j * B
                if j:
                    leave(j - 1).start()
                ljj = jnp.where(right, ut[...], 0.0).T + LD[...]
                L[lo:lo + B, lo:lo + B] = ljj
                if j + 1 < nb:
                    hi = lo + B
                    ms = split3(jnp.where(tri, ut[...], 0.0))
                    w = W[hi:n, :] if j else a(hi, n, lo)
                    x = nt6(split3(w), ms)
                    L[hi:n, lo:hi] = x
                    S1[hi:n, lo:hi], S2[hi:n, lo:hi], S3[hi:n, lo:hi] = split3(x)
                    w = a(hi, n, hi) - nt6([s[hi:n, 0:hi] for s in (S1, S2, S3)],
                                           [s[hi:hi + B, 0:hi] for s in (S1, S2, S3)])
                    rt[...] = w[:B] + ridge_at(hi)
                    W[hi:n, :] = w
        return carry
    lax.fori_loop(0, nb, step, 0)
    for j in range(nb - 1):
        leave(j).wait()
    leave(nb - 1).start()
    leave(nb - 1).wait()


def chol(h, g, e, misc):
    n = misc.shape[1]
    return pl.pallas_call(
        functools.partial(chol_kernel, n=n),
        out_shape=pltpu.HBM((n // 2, n), jnp.float32),
        in_specs=[SM] + [VM] * 3,
        out_specs=HB,
        scratch_shapes=[pltpu.VMEM((B, B), jnp.float32), pltpu.VMEM((B, B), jnp.float32),
                        pltpu.VMEM((n, n), jnp.float32)] + [pltpu.VMEM((n, n), jnp.bfloat16)] * 3
        + [pltpu.VMEM((4 * B, 2 * B), jnp.bfloat16), pltpu.VMEM((n, B), jnp.float32), pltpu.VMEM((B, B), jnp.float32), DMA((n // B,))],
        cost_estimate=pl.CostEstimate(flops=10**9, bytes_accessed=8 * 2**20, transcendentals=0),
        compiler_params=pltpu.CompilerParams(vmem_limit_bytes=24 * 2**20),
    )(h, g, e, misc)


def feat(pts, wf, turns, scale):
    dot = jnp.dot(pts, wf, preferred_element_type=jnp.float32)
    t = dot * (0.5 / math.pi) + turns
    v = 0.25 - jnp.abs(t - jnp.round(t))
    w = v * v
    poly = w * (scale * SIN[-1]) + scale * SIN[-2]
    for c in SIN[-3::-1]:
        poly = poly * w + scale * c
    return (v * poly).astype(jnp.bfloat16)


def tn(x, y):
    return lax.dot_general(x, y, (((0,), (0,)), ((), ())), preferred_element_type=jnp.float32)


def win_kernel(*refs, nc, acc, scale, rows):
    h_ref = refs[0]
    if acc:
        wf, misc, a0 = refs[1:4]
        chunks = refs[4:4 + nc]
        out, far, phi, sems = refs[4 + nc:]
        din, full = wf.shape
        half = full // 2
    else:
        fr, fp = refs[1:3]
        chunks = refs[3:3 + nc]
        out, far, wf, misc, phi, sems = refs[3 + nc:]
        din, full = wf.shape
        half = full // 2
        first = h_ref[0] == 0
        wf[:, :half] = jnp.where(first, fr[:din, :], fp[:din, :])
        wf[:, half:] = jnp.where(first, fp[:din, :], fr[:din, :])
        for which, at in ((1, 0), (0, 8)):
            mine, other = extra(fr, which), extra(fp, which)
            row = jnp.concatenate([jnp.where(first, mine, other), jnp.where(first, other, mine)], axis=1)
            misc[at:at + 1, :] = row
        misc[1:2, :half] = extra(fr, 1)
        misc[1:2, half:] = extra(fp, 1)
    turns = misc[8:9, :]
    col0 = pl.multiple_of(h_ref[0] * half, half)

    def leave(i, what):
        at = pl.ds(i * rows, rows)
        last = pl.ds(nc * rows + i * EXTRA, EXTRA)
        src, dst = (
            (chunks[i].at[pl.ds(0, rows), :], far.at[at, pl.ds(half, din)]),
            (chunks[i].at[pl.ds(rows, EXTRA), :], far.at[last, pl.ds(half, din)]),
            (phi.at[at, pl.ds(col0, half)], far.at[at, pl.ds(0, half)]),
        )[what]
        return pltpu.make_async_copy(src, dst, sems.at[i, what])

    for i in range(nc):
        leave(i, 0).start()
        leave(i, 1).start()
    for i in range(nc):
        pts = chunks[i][:rows, :]
        for c in range(0, full, NT):
            phi[i * rows:(i + 1) * rows, c:c + NT] = feat(pts, wf[:, c:c + NT], turns[:, c:c + NT], scale)
        if i:
            leave(i - 1, 2).start()
    for c in range(full // NT):
        at = strip(full, c)
        r = tn(phi[:, c * NT:], phi[:, c * NT:(c + 1) * NT])
        if acc:
            r = r + a0[at:at + r.shape[0], :]
        out[at:at + r.shape[0], :] = r
        if c == 0:
            leave(nc - 1, 2).start()
    for i in range(nc):
        for what in range(3):
            leave(i, what).wait()


def win(h, weights, chunks, before, scale, rows):
    acc = before is not None
    f32, bf = jnp.float32, jnp.bfloat16
    if acc:
        din, full = weights[0].shape
    else:
        din, full = weights[0].shape[0] - EXTRA, 2 * weights[0].shape[1]
    nc = len(chunks)
    args = [h, *weights] + ([before] if acc else []) + list(chunks)
    shapes = [((strip(full, full // NT), NT), f32), ((nc * (rows + EXTRA), full // 2 + din), bf)]
    if not acc:
        shapes += [((din, full), bf), ((16, full), f32)]
    return pl.pallas_call(
        functools.partial(win_kernel, nc=nc, acc=acc, scale=scale, rows=rows),
        out_shape=[(pltpu.HBM if i == 1 else pltpu.VMEM)(s, d) for i, (s, d) in enumerate(shapes)],
        in_specs=[SM] + [VM] * (len(args) - 1),
        out_specs=[HB if i == 1 else VM for i in range(len(shapes))],
        scratch_shapes=[pltpu.VMEM((nc * rows, full), bf), DMA((nc, 3))],
        cost_estimate=pl.CostEstimate(flops=nc * rows * full * (din + full * 5 // 8) * 2,
                                      bytes_accessed=4 * 2**20, transcendentals=0),
        compiler_params=pltpu.CompilerParams(vmem_limit_bytes=20 * 2**20),
    )(*args)


def col_kernel(f_ref, fc, misc, *refs, scale, rows):
    n = (len(refs) - 4) // 2
    g, pr, phi = refs[n:n + 3]
    parts, sems = refs[n + 3:-1], refs[-1]
    copies = [pltpu.make_async_copy(refs[i], parts[i], sems.at[i]) for i in range(n)]
    for copy in copies:
        copy.start()
    din, width = fc.shape[0] - EXTRA, fc.shape[1]
    half = misc.shape[1] // 2
    turns = extra(fc, 0)
    counts = [p.shape[0] // (rows + EXTRA) for p in parts]
    base = 0
    for copy, p, m in zip(copies, parts, counts):
        copy.wait()
        for i in range(m):
            for c in range(0, width, NT):
                phi[base + i * rows:base + (i + 1) * rows, c:c + NT] = feat(
                    p[i * rows:(i + 1) * rows, half:], fc[:din, c:c + NT], turns[:, c:c + NT], scale)
        base += m * rows
    ii = lax.broadcasted_iota(jnp.int32, (half, NT), 0)
    jj = lax.broadcasted_iota(jnp.int32, (half, NT), 1)
    same = f_ref[0] != 0
    ridge = misc[1:2, :half]
    for c in range(0, width, NT):
        total = jnp.where((ii == jj + c) & same, ridge[:, c:c + NT], 0.0)
        base = 0
        for p, m in zip(parts, counts):
            total = total + tn(p[:m * rows, :half], phi[base:base + m * rows, c:c + NT])
            base += m * rows
        g[:, c:c + NT] = total
    total = jnp.zeros((8, half), jnp.float32)
    for p, m in zip(parts, counts):
        t = [p[m * rows + i * EXTRA:m * rows + (i + 1) * EXTRA, half:][:8] for i in range(m)]
        total = total + jnp.dot(jnp.concatenate(t, axis=1), p[:m * rows, :half], preferred_element_type=jnp.float32)
    pr[...] = total


def col(flag, fc, misc, parts, scale, rows):
    width = fc.shape[1]
    half = misc.shape[1] // 2
    args = [flag, fc, misc, *parts]
    total = sum(p.shape[0] // (rows + EXTRA) * rows for p in parts)
    return pl.pallas_call(
        functools.partial(col_kernel, scale=scale, rows=rows),
        out_shape=[jax.ShapeDtypeStruct((half, width), jnp.float32), jax.ShapeDtypeStruct((8, half), jnp.float32)],
        in_specs=[SM, VM, VM] + [HB] * len(parts),
        out_specs=[VM] * 2,
        scratch_shapes=[pltpu.VMEM((total, width), jnp.bfloat16)]
        + [pltpu.VMEM(p.shape, p.dtype) for p in parts] + [DMA((len(parts),))],
        cost_estimate=pl.CostEstimate(flops=8 * 10**9, bytes_accessed=12 * 2**20, transcendentals=0),
        compiler_params=pltpu.CompilerParams(vmem_limit_bytes=24 * 2**20),
    )(*args)


def prep_kernel(p, t, f, ph, ri, pack, fpack):
    rows, din = p.shape[0], f.shape[0]
    pack[:rows, :] = p[...]
    pack[rows:, :] = jnp.concatenate([t[...], jnp.zeros_like(t[...])], axis=0)
    fpack[:din, :] = f[...]
    x = list(split3(ph[...] * (0.5 / math.pi))) + list(split3(ri[...]))
    pad = jnp.zeros((EXTRA - 6, f.shape[1]), jnp.float32)
    fpack[din:, :] = jnp.concatenate([v.astype(jnp.float32) for v in x] + [pad], axis=0).astype(jnp.bfloat16)


def prep(points, targets, freqs, phase, ridge):
    rows, din = points.shape
    w = phase.shape[0]
    return pl.pallas_call(
        prep_kernel,
        out_shape=[pltpu.VMEM((rows + EXTRA, din), jnp.bfloat16),
                   pltpu.VMEM((freqs.shape[0] + EXTRA, w), jnp.bfloat16)],
        in_specs=[VM] * 5,
        out_specs=[VM] * 2,
    )(points, targets, freqs, phase.reshape(1, w), ridge.reshape(1, w))


def shards(points, freqs, phase, ridge, targets):
    nd = lax.axis_size("dp")
    nf = lax.axis_size("feat")
    fi = lax.axis_index("feat")
    di = lax.axis_index("dp")
    nz = nd // 2
    rows = points.shape[0]
    scale = math.sqrt(2.0 / (rows * nd))

    def zshift(x, s):
        return lax.ppermute(x, "dp", [(2 * z + c, 2 * ((z + s) % nz) + c) for z in range(nz) for c in range(2)])

    def sibling(x):
        return lax.ppermute(x, "dp", [(i, i ^ 1) for i in range(nd)])

    def partner(x):
        return lax.ppermute(x, "feat", [(i, i ^ 1) for i in range(nf)])

    def swap(x):
        return lax.ppermute(x, ("dp", "feat"), [(i * nf + j, j * nd + i) for i in range(nd) for j in range(nf)])

    pack, fr = prep(points, targets, freqs, phase, ridge)
    u1, d1, u2, d2 = zshift(pack, 1), zshift(pack, -1), zshift(pack, 2), zshift(pack, -2)
    fp = partner(fr)
    u3, d3, u4 = zshift(u2, 1), zshift(d2, -1), zshift(u2, 2)
    h = jnp.reshape(fi % 2, (1,)).astype(jnp.int32)
    late = lax.optimization_barrier((fr, u2, d2))[0]
    fc = swap(late)
    g, o1, wf, misc = win(h, (fr, fp), [pack, u1, d1, u2, d2], None, scale, rows)
    s1 = sibling(o1)
    g, o2 = win(h, (wf, misc), [u3, d3, u4], g, scale, rows)
    e = sibling(g)
    s2 = sibling(o2)
    factor_rows = chol(h, g, e, misc)
    flag = jnp.reshape(fi == di, (1,)).astype(jnp.int32)
    flag, factor_rows = lax.optimization_barrier((flag, factor_rows))
    gram_tile, projected = col(flag, fc, misc, (o2, o1, s2, s1), scale, rows)
    return (gram_tile, projected, factor_rows)


def solution(mesh):
    in_specs = (P("dp", None), P(None, "feat"), P("feat"), P("feat"), P(None, "dp"))
    out_specs = (P("feat", "dp"), P(None, "feat"), P("feat", None))
    return jax.shard_map(shards, mesh=mesh, in_specs=in_specs, out_specs=out_specs, check_vma=False)
```
